128 devices in a mesh: rows: 128 (over x, z, y, core).
Axes of the slice: x: 4, y: 4, z: 4, core: 2. Of those that a mesh axis runs over, the one named last changes fastest.
Arguments:
- design: bfloat16 [524288, 1024], P('rows'), may hold values from -6 to 6
- weights: float32 [1024], replicated, may hold values from -0.1875 to 0.1875
- labels: int32 [524288], P('rows'), may hold values from 0 to 1
- signs: int32 [524288], P('rows'), may hold values from 0 to 1
- sample_rows: int32 [2048], replicated, may hold values from 0 to 524287
Outputs:
- gradient: float32 [1024], replicated
- newton_step: float32 [1024], replicated
- losses: float32 [4], replicated
The draws below stay inside these ranges and needn't reach their ends.
All inputs are finite; a program needn't handle non-finite values.
Results may differ from the reference program's by a relative error of at most 0.00085.
The reference program's roundings to bfloat16 on the way count: a program that leaves them out, or rounds other values in their place, can miss the bound.
Values may be sent and summed in bfloat16 or wider, within the bound.
No kernel may reach another device: no remote copies, remote signals or barrier semaphores. Data moves between devices by JAX's collectives and lax.ppermute only.
A program may use at most 128 MiB of HBM per device.

```python
import jax
import jax.numpy as jnp
from jax import lax

WIDTH = 1024
ROWS_DEV = 4096
TOTAL_ROWS = 524288
SKETCH = 2048
N_ROWS = 128


def plant(drawn, rng, least, largest):
    longest = drawn.shape.index(max(drawn.shape))
    spots = []
    for shift in (0, 1):
        where = [jax.random.randint(jax.random.fold_in(rng, axis), (), 0, length) for axis, length in enumerate(drawn.shape)]
        where[longest] = (where[longest] + shift) % drawn.shape[longest]
        spots.append(tuple(where))
    return drawn.at[spots[0]].set(least).at[spots[1]].set(largest)


def shard_levels(rng, shape, split, low, largest):
    level, own = 1.0, jax.random.fold_in(rng, 6)
    for dim, parts in split:
        heights = jnp.exp(jax.random.uniform(jax.random.fold_in(own, dim), (parts,), jnp.float32, low / len(split), largest / len(split)))
        level = level * jnp.repeat(heights, shape[dim] // parts).reshape([-1 if axis == dim else 1 for axis in range(len(shape))])
    return level


def centred(key, shape, deviation, reach, cuts=(), kind=jnp.bfloat16):
    entries = deviation * jax.random.normal(key, shape, jnp.float32)
    if cuts:
        entries = entries * shard_levels(key, shape, cuts, -0.22, 0.18)
    return jnp.clip(entries, -reach, reach).astype(kind)


def setup_inputs(seed: int = 0) -> dict:
    keys = jax.random.split(jax.random.key(seed), 6)
    return {
        "design": centred(keys[0], (TOTAL_ROWS, WIDTH), 1.0, 6.0, ((0, 128),)),
        "weights": centred(keys[1], (WIDTH,), WIDTH ** -0.5, 0.1875, (), jnp.float32),
        "labels": plant(jax.random.randint(keys[2], (TOTAL_ROWS,), 0, 2), jax.random.fold_in(keys[2], 1), 0, 1).astype(jnp.int32),
        "signs": plant(jax.random.randint(keys[3], (TOTAL_ROWS,), 0, 2), jax.random.fold_in(keys[3], 1), 0, 1).astype(jnp.int32),
        "sample_rows": plant(jax.random.randint(keys[4], (SKETCH,), 0, TOTAL_ROWS), jax.random.fold_in(keys[4], 1), 0, TOTAL_ROWS - 1).astype(jnp.int32),
    }


ridge = 0.05

def hadamard(order_size):
    bits = order_size.bit_length() - 1
    row_index = lax.broadcasted_iota(jnp.int32, (order_size, order_size), 0)
    col_index = lax.broadcasted_iota(jnp.int32, (order_size, order_size), 1)
    parity = jnp.zeros((order_size, order_size), jnp.int32)
    for bit_number in range(bits):
        parity = parity + (row_index >> bit_number & 1) * (col_index >> bit_number & 1)
    return (1 - 2 * (parity % 2)).astype(jnp.float32)

def local_transform(scaled):
    rows_here, width = scaled.shape
    bits = rows_here.bit_length() - 1
    low_order = 1 << bits // 2
    high_order = rows_here // low_order
    high_matrix = hadamard(high_order).astype(jnp.bfloat16)
    first = jnp.dot(high_matrix.astype(jnp.float32), scaled.reshape(high_order, low_order * width).astype(jnp.float32), preferred_element_type=jnp.float32)
    low_matrix = hadamard(low_order)
    second = jnp.einsum('bx,axd->abd', low_matrix, first.reshape(high_order, low_order, width), precision=lax.Precision.HIGHEST)
    return second.reshape(rows_here, width)

def reference(design, weights, labels, signs, sample_rows):
    total_rows, width = design.shape
    margins = jnp.dot(design.astype(jnp.float32), weights.astype(jnp.bfloat16).astype(jnp.float32), preferred_element_type=jnp.float32)
    prob = jax.nn.sigmoid(margins)
    target = labels.astype(jnp.float32)
    misfit = (prob - target).astype(jnp.bfloat16)
    gradient = jnp.dot(misfit.astype(jnp.float32), design.astype(jnp.float32), preferred_element_type=jnp.float32) / total_rows + ridge * weights
    factor_rows = (1.0 - 2.0 * signs.astype(jnp.float32)) * jnp.sqrt(prob * (1.0 - prob))
    owner = sample_rows // ROWS_DEV
    local_rows = sample_rows % ROWS_DEV
    norm_factor = 1.0 / jnp.sqrt(jnp.float32(sample_rows.shape[0]))
    dev_bits = N_ROWS.bit_length() - 1

    def accumulate(carry, inputs):
        block, block_factor, device = inputs
        scaled = (block * block_factor[:, None]).astype(jnp.bfloat16)
        mixed = local_transform(scaled)
        parity = jnp.zeros(owner.shape, jnp.int32)
        for bit_number in range(dev_bits):
            parity = parity + (owner >> bit_number & 1) * (device >> bit_number & 1)
        coefs = (1 - 2 * (parity % 2)).astype(jnp.float32) * norm_factor
        return (carry + jnp.take(mixed, local_rows, axis=0) * coefs[:, None], None)
    blocks = design.reshape(N_ROWS, ROWS_DEV, width)
    factors = factor_rows.reshape(N_ROWS, ROWS_DEV)
    devices_list = jnp.arange(N_ROWS, dtype=jnp.int32)
    start_value = jnp.zeros((sample_rows.shape[0], width), jnp.float32)
    sketch_sum, unused = lax.scan(accumulate, start_value, (blocks, factors, devices_list))
    sketch = sketch_sum.astype(jnp.bfloat16)
    gram = jnp.dot(sketch.T.astype(jnp.float32), sketch.astype(jnp.float32), preferred_element_type=jnp.float32)
    hessian = gram / total_rows + ridge * jnp.eye(width, dtype=jnp.float32)
    cholesky_factor = jnp.linalg.cholesky(hessian)
    newton_step = jax.scipy.linalg.cho_solve((cholesky_factor, True), gradient)
    along = jnp.dot(design.astype(jnp.float32), newton_step.astype(jnp.bfloat16).astype(jnp.float32), preferred_element_type=jnp.float32)
    lengths = jnp.array([1.0, 0.5, 0.25, 0.125], jnp.float32)
    trial = margins[None, :] - lengths[:, None] * along[None, :]
    row_loss = jnp.logaddexp(0.0, trial) - target[None, :] * trial
    moved = weights[None, :] - lengths[:, None] * newton_step[None, :]
    losses = lax.optimization_barrier(jnp.sum(row_loss, axis=1)) / total_rows + 0.5 * ridge * lax.optimization_barrier(jnp.sum(moved * moved, axis=1))
    return (gradient, newton_step, losses)
```

```python
import functools

import jax
import jax.numpy as jnp
from jax import lax
from jax.experimental import pallas as pl
from jax.experimental.pallas import tpu as pltpu
from jax.sharding import Mesh
from jax.sharding import PartitionSpec as P

ROWS = ("rows_0", "rows_1", "rows_2", "rows_3")

ridge = 0.05

PARTS = ((0, 3, (0, 1, 2)), (3, 6, (1, 2, 0)), (6, 8, (2, 0, 1)))


def shift(x, axis, k):
    size = 2 if axis == 3 else 4
    return lax.ppermute(x, ROWS[axis], [(i, (i + k) % size) for i in range(size)])


def sum_of_four(x):
    return (x[0] + x[2]) + (x[1] + x[3])


HI = lax.Precision.HIGHEST
NB = 128

def row_of(x, j):
    return jnp.broadcast_to(x[j:j + 1, :], x.shape)

def col_of(x, j):
    return jnp.broadcast_to(x[:, j:j + 1], x.shape)

def invert_block(block):
    tiles = [block[8 * i:8 * i + 8, :] for i in range(16)]
    lane = lax.broadcasted_iota(jnp.int32, (8, NB), 1)
    sub = lax.broadcasted_iota(jnp.int32, (8, NB), 0)
    at_row = [sub == j for j in range(8)]
    for p in range(16):
        inside = lane // 8 == p
        cols = [[None if i == p else col_of(tiles[i], 8 * p + j) for j in range(8)] for i in range(16)]
        own = [col_of(tiles[p], 8 * p + j) for j in range(8)]
        panel = jnp.where(inside, jnp.where(lane - 8 * p == sub, 1.0, 0.0), tiles[p])
        for j in range(8):
            inv = 1.0 / row_of(own[j], j)
            line = row_of(panel, j) * inv
            panel = jnp.where(at_row[j], line, panel - own[j] * line)
            for k in range(j + 1, 8):
                lk = row_of(own[k], j) * inv
                own[k] = jnp.where(at_row[j], lk, own[k] - own[j] * lk)
        lines = [row_of(panel, j) for j in range(8)]
        for i in range(16):
            if i == p:
                continue
            t = jnp.where(inside, 0.0, tiles[i])
            for j in range(8):
                t = t - cols[i][j] * lines[j]
            tiles[i] = t
        tiles[p] = panel
    return jnp.concatenate(tiles, 0)

def nn(a, b):
    return lax.dot_general(a, b, (((1,), (0,)), ((), ())), precision=HI, preferred_element_type=jnp.float32)

def nt(a, b):
    return lax.dot_general(a, b, (((1,), (1,)), ((), ())), precision=HI, preferred_element_type=jnp.float32)

def factor_solve(h_ref, x_ref, n):
    blocks = n // NB
    for k in range(blocks):
        kc = slice(k * NB, (k + 1) * NB)
        s = (k + 1) * NB
        inv = invert_block(h_ref[kc, kc])
        below = h_ref[s:n + 8, kc]
        w = nn(below, inv)
        c = s
        while c < n:
            wd = min(256, n - c)
            h_ref[c:n + 8, c:c + wd] -= nt(w[c - s:, :], below[c - s:c - s + wd, :])
            c += wd
        h_ref[s:n + 8, kc] = w
    for k in reversed(range(blocks)):
        kc = slice(k * NB, (k + 1) * NB)
        s = (k + 1) * NB
        y = h_ref[n:n + 8, kc]
        if s < n:
            y = y - nn(x_ref[:, s:], h_ref[s:n, kc])
        x_ref[:, kc] = y


def solve_kernel(total, parts, where_ref, *refs):
    halves, (g_ref, x_ref, s_ref, h_ref) = refs[: 2 * len(parts)], refs[2 * len(parts):]
    n = s_ref.shape[1]
    for i, (low, high, order) in enumerate(parts):
        for partner in range(2):
            src = halves[2 * i + partner]
            core = where_ref[3] if partner == 0 else 1 - where_ref[3]

            def place(j, carry, src=src, core=core, order=order, low=low, high=high):
                rel = (j // 16, j // 4 % 4, j % 4)
                at = [0, 0, 0]
                for axis, r in zip(order, rel):
                    at[axis] = (r + where_ref[axis]) % 4
                to = (((core * 4 + at[0]) * 4 + at[1]) * 4 + at[2]) * 16
                for c in range(high - low):
                    got = src[pl.ds(pl.multiple_of((j * (high - low) + c) * 16, 16), 16), :]
                    s_ref[pl.ds(pl.multiple_of(to, 16), 16), (low + c) * 128:(low + c + 1) * 128] = got
                return carry

            lax.fori_loop(0, 64, place, 0)
    for c in range(0, n, 256):
        gram = lax.dot_general(
            s_ref[:, c:], s_ref[:, c:c + 256], (((0,), (0,)), ((), ())), preferred_element_type=jnp.float32
        )
        r = lax.broadcasted_iota(jnp.int32, gram.shape, 0)
        q = lax.broadcasted_iota(jnp.int32, gram.shape, 1)
        h_ref[c:n, c:c + 256] = gram / total + jnp.where(r == q, ridge, 0.0)
    h_ref[n:n + 8, :] = jnp.broadcast_to(g_ref[...], (8, n))
    factor_solve(h_ref, x_ref, n)


def solve(pieces, gradient, where, total):
    n = gradient.shape[0]
    rows = 2 * 64 * 16
    vmem = pl.BlockSpec(memory_space=pltpu.VMEM)
    return pl.pallas_call(
        functools.partial(solve_kernel, total, PARTS),
        out_shape=jax.ShapeDtypeStruct((8, n), jnp.float32),
        in_specs=[pl.BlockSpec(memory_space=pltpu.SMEM)] + [vmem] * (len(pieces) + 1),
        out_specs=vmem,
        scratch_shapes=[pltpu.VMEM((rows, n), jnp.bfloat16), pltpu.VMEM((n + 8, n), jnp.float32)],
        compiler_params=pltpu.CompilerParams(vmem_limit_bytes=48 << 20),
        name="solve",
    )(where, *pieces, gradient[None, :])[0]


def reduce_over_devices(mine, other, grad):
    with_grad = len(PARTS) - 1
    blocks = list(mine)
    g = grad

    def exchange(i, x, axis, k):
        flat = x.reshape(-1, x.shape[-1])
        if i != with_grad:
            return shift(flat, axis, k).reshape(x.shape), None
        got = shift(jnp.concatenate([flat, g], 0), axis, k)
        return got[: flat.shape[0]].reshape(x.shape), got[flat.shape[0]:]

    for i in range(len(PARTS)):
        got, got_g = exchange(i, other[i], 3, 1)
        blocks[i] = blocks[i] + got
        if got_g is not None:
            new_g = g + got_g
    g = new_g
    left = [[0, 1, 2] for _ in PARTS]
    for stage in range(2):
        for i, (low, high, order) in enumerate(PARTS):
            axis = order[stage]
            pos = left[i].index(axis)
            terms, terms_g = [lax.index_in_dim(blocks[i], 0, pos, False)], [g]
            for k in (1, 2, 3):
                got, got_g = exchange(i, lax.index_in_dim(blocks[i], k, pos, False), axis, k)
                terms.append(got)
                terms_g.append(got_g)
            blocks[i] = sum_of_four(terms)
            left[i].remove(axis)
            if i == with_grad:
                new_g = sum_of_four(terms_g)
        g = new_g
    for i, (low, high, order) in enumerate(PARTS):
        axis = order[2]
        terms, terms_g = [blocks[i]], [g]
        for k in (1, 2, 3):
            got, got_g = exchange(i, blocks[i], axis, k)
            terms.append(jnp.roll(got, -k, 0))
            terms_g.append(got_g)
        blocks[i] = sum_of_four(terms).astype(jnp.bfloat16)
        if i == with_grad:
            new_g = sum_of_four(terms_g)
    g = new_g
    for stage in (1, 0):
        for i, (low, high, order) in enumerate(PARTS):
            axis = order[stage]
            flat = blocks[i].reshape(-1, 128)
            got = [flat] + [shift(flat, axis, k) for k in (3, 2, 1)]
            blocks[i] = jnp.concatenate(got, 0)
    pieces = []
    for b in blocks:
        pieces += [b, shift(b, 3, 1)]
    return pieces, g


def sum_over_devices(x):
    x = x + shift(x, 3, 1)
    for axis in range(3):
        x = sum_of_four([x] + [shift(x, axis, k) for k in (1, 2, 3)])
    return x


def front_kernel(where_ref, row_ref, coef_ref, w_ref, label_ref, sign_ref, x_ref,
                 margin_ref, grad_ref, a_ref, b_ref, c_ref, had_ref, mix_ref):
    step = pl.program_id(0)
    sub_blocks = x_ref.shape[0] // 256

    @pl.when(step == 0)
    def _():
        i = lax.broadcasted_iota(jnp.int32, (256, 256), 0)
        j = lax.broadcasted_iota(jnp.int32, (256, 256), 1)
        v = i & j
        v = v ^ (v >> 4)
        v = v ^ (v >> 2)
        v = (v ^ (v >> 1)) & 1
        had_ref[...] = jnp.where(v == 0, 1.0, -1.0).astype(jnp.bfloat16)
        grad_ref[...] = jnp.zeros_like(grad_ref)

    for sb in range(sub_blocks):
        rows = slice(sb * 256, (sb + 1) * 256)
        x = x_ref[rows, :]
        margin = lax.dot_general(w_ref[...], x, (((1,), (1,)), ((), ())), preferred_element_type=jnp.float32)
        prob = jax.nn.sigmoid(margin)
        target = label_ref[:, rows].astype(jnp.float32)
        misfit = (prob - target).astype(jnp.bfloat16)
        spread = prob * (1.0 - prob)
        factor = jnp.where(spread > 0.0, jnp.sqrt(spread), 0.0)
        factor = (1.0 - 2.0 * sign_ref[:, rows].astype(jnp.float32)) * factor
        margin_ref[:, rows] = margin[:1, :]
        grad_ref[...] += jnp.dot(misfit, x, preferred_element_type=jnp.float32)
        column = jnp.broadcast_to(factor[:1, :], (128, 256)).T
        for c in range(8):
            cols = slice(c * 128, (c + 1) * 128)
            scaled = (x[:, cols].astype(jnp.float32) * column).astype(jnp.bfloat16)
            first = jnp.dot(had_ref[...], scaled, preferred_element_type=jnp.float32)
            at = (step * sub_blocks + sb) * 32
            mix_ref[pl.ds(at, 32), c * 8:(c + 1) * 8, :] = first.reshape(32, 8, 128)

    @pl.when(step == pl.num_programs(0) - 1)
    def _():
        def butterflies(t, carry):
            for c in range(8):
                cols = slice(c * 8, (c + 1) * 8)
                v = [mix_ref[t + 32 * k, cols, :] for k in range(16)]
                for bit in (1, 2, 4, 8):
                    v = [v[k] + v[k ^ bit] if not k & bit else v[k ^ bit] - v[k] for k in range(16)]
                for k in range(16):
                    mix_ref[t + 32 * k, cols, :] = v[k]
            return carry

        lax.fori_loop(0, 32, butterflies, 0)

        def pick(p, carry):
            core = (p // 64) ^ where_ref[3]
            chip = 0
            for axis, unit in ((0, 16), (1, 4), (2, 1)):
                chip = chip * 4 + ((p // unit + where_ref[axis]) & 3)
            base = (chip * 2 + core) * 16
            for s in range(16):
                row = row_ref[base + s]
                coef = coef_ref[base + s]
                for out, low, count in ((a_ref, 0, 3), (b_ref, 24, 3), (c_ref, 48, 2)):
                    got = mix_ref[row // 8, pl.ds(low + row % 8, count, stride=8), :]
                    out[p, pl.ds(s, count, stride=16), :] = got * coef
            return carry

        lax.fori_loop(0, 128, pick, 0)


def front(design, weights, labels, signs, rows, coefs, where):
    rows_here, width = design.shape
    block = 512
    smem = pl.BlockSpec(memory_space=pltpu.SMEM)
    whole = lambda *shape: pl.BlockSpec(shape, lambda i: (0,) * len(shape))
    w = jnp.broadcast_to(weights.astype(jnp.bfloat16)[None, :], (8, width))
    picked = [(128, 48, 128), (128, 48, 128), (128, 32, 128)]
    return pl.pallas_call(
        front_kernel,
        grid=(rows_here // block,),
        out_shape=[
            jax.ShapeDtypeStruct((1, rows_here), jnp.float32),
            jax.ShapeDtypeStruct((8, width), jnp.float32),
        ] + [jax.ShapeDtypeStruct(s, jnp.float32) for s in picked],
        in_specs=[
            smem, smem, smem,
            whole(8, width),
            pl.BlockSpec((1, block), lambda i: (0, i)),
            pl.BlockSpec((1, block), lambda i: (0, i)),
            pl.BlockSpec((block, width), lambda i: (i, 0)),
        ],
        out_specs=[pl.BlockSpec((1, block), lambda i: (0, i)), whole(8, width)] + [whole(*s) for s in picked],
        scratch_shapes=[pltpu.VMEM((256, 256), jnp.bfloat16), pltpu.VMEM((512, 64, 128), jnp.float32)],
        compiler_params=pltpu.CompilerParams(vmem_limit_bytes=48 << 20),
        name="front",
    )(where, rows, coefs, w, labels[None, :], signs[None, :], design)


def body(design, weights, labels, signs, sample_rows):
    rows_here, width = design.shape
    device_count = lax.axis_size(ROWS)
    device_index = lax.axis_index(ROWS)
    where = jnp.stack([lax.axis_index(a) for a in ROWS])
    total_rows = rows_here * device_count
    norm_factor = 1.0 / jnp.sqrt(jnp.float32(sample_rows.shape[0]))
    parity = (sample_rows // rows_here) & device_index
    for bits in (4, 2, 1):
        parity = parity ^ (parity >> bits)
    coefs = (1 - 2 * (parity & 1)).astype(jnp.float32) * norm_factor
    margins, grad_part, *picked = front(
        design, weights, labels, signs, sample_rows % rows_here, coefs, where
    )
    picked = [p.reshape(2, 4, 4, 4, -1, 128) for p in picked]
    mine = [p[0] for p in picked]
    other = [p[1] for p in picked]
    pieces, grad = reduce_over_devices(mine, other, grad_part[0].reshape(8, 128))
    gradient = grad.reshape(-1) / total_rows + ridge * weights
    newton_step = solve(pieces, gradient, where, float(total_rows))
    along = jnp.dot(design, newton_step.astype(jnp.bfloat16), preferred_element_type=jnp.float32)
    lengths = jnp.array([1.0, 0.5, 0.25, 0.125], jnp.float32)
    margins = margins[0]
    target = labels.astype(jnp.float32)
    trial = margins[None, :] - lengths[:, None] * along[None, :]
    row_loss = jnp.logaddexp(0.0, trial) - target[None, :] * trial
    loss_total = sum_over_devices(jnp.sum(row_loss, axis=1))
    moved = weights[None, :] - lengths[:, None] * newton_step[None, :]
    losses = loss_total / total_rows + 0.5 * ridge * jnp.sum(moved * moved, axis=1)
    return (gradient, newton_step, losses)


def solution(mesh):
    torus = Mesh(mesh.devices.reshape(4, 4, 4, 2), ROWS)
    in_specs = (P(ROWS, None), P(), P(ROWS), P(ROWS), P())
    out_specs = (P(), P(), P())
    return jax.shard_map(body, mesh=torus, in_specs=in_specs, out_specs=out_specs, check_vma=False)
```

```python
import functools

import jax
import jax.numpy as jnp
from jax import lax
from jax.experimental import pallas as pl
from jax.experimental.pallas import tpu as pltpu
from jax.sharding import Mesh
from jax.sharding import PartitionSpec as P

ROWS = ("rows_0", "rows_1", "rows_2", "rows_3")

ridge = 0.05

PARTS = ((0, 4, (0, 1)), (4, 8, (1, 0)))


def shift(x, axis, k):
    size = 2 if axis == 3 else 4
    return lax.ppermute(x, ROWS[axis], [(i, (i + k) % size) for i in range(size)])


def sum_of_four(x):
    return (x[0] + x[2]) + (x[1] + x[3])


HI = lax.Precision.HIGHEST
NB = 128

def row_of(x, j):
    return jnp.broadcast_to(x[j:j + 1, :], x.shape)

def col_of(x, j):
    return jnp.broadcast_to(x[:, j:j + 1], x.shape)

def invert_block(block):
    lane = lax.broadcasted_iota(jnp.int32, (8, NB), 1)
    sub = lax.broadcasted_iota(jnp.int32, (8, NB), 0)
    lanes = lax.broadcasted_iota(jnp.int32, (NB, NB), 1)
    rows = lax.broadcasted_iota(jnp.int32, (NB, NB), 0)
    real = lane < NB
    for p in range(4):
        tiles = [block[32 * p + 8 * t:32 * p + 8 * t + 8, :] for t in range(4)]
        for q in range(2):
            base = 32 * p + 16 * q
            inside = (lane >= base) & (lane < base + 16)
            mine, others = (2 * q, 2 * q + 1), (2 - 2 * q, 3 - 2 * q)
            own = [[jnp.where(real, col_of(tiles[t], base + j), 0.0) for t in mine] for j in range(16)]
            cols = {i: [col_of(tiles[i], base + j) for j in range(16)] for i in others}
            panel = [
                jnp.where(inside, jnp.where(lane - base == sub + 8 * h, 1.0, 0.0), tiles[mine[h]]) for h in range(2)
            ]
            for j in range(0, 16, 2):
                half, r = j // 8, j % 8
                first, second = own[j], own[j + 1]
                a, b = row_of(first[half], r), row_of(second[half], r)
                c, d = row_of(first[half], r + 1), row_of(second[half], r + 1)
                inv = 1.0 / (a * d - b * c)
                a, b, c, d = d * inv, b * inv, c * inv, a * inv

                def eliminate(x):
                    top, low = row_of(x[half], r), row_of(x[half], r + 1)
                    top, low = a * top - b * low, d * low - c * top
                    out = [x[h] - first[h] * top - second[h] * low for h in range(2)]
                    out[half] = jnp.where(sub == r, top, jnp.where(sub == r + 1, low, out[half]))
                    return out

                for k in range(j + 2, 16):
                    own[k] = eliminate(own[k])
                panel = eliminate(panel)
            lines = [row_of(panel[j // 8], j % 8) for j in range(16)]
            for i in others:
                t = jnp.where(inside, 0.0, tiles[i])
                for j in range(16):
                    t = t - cols[i][j] * lines[j]
                tiles[i] = t
            tiles[mine[0]], tiles[mine[1]] = panel
        here = (rows >= 32 * p) & (rows < 32 * p + 32)
        inside = (lanes >= 32 * p) & (lanes < 32 * p + 32)
        done = jnp.concatenate([block[:32 * p, :]] * (p > 0) + tiles + [block[32 * p + 32:, :]] * (p < 3), 0)
        rest = jnp.where(inside, 0.0, block) - nn(jnp.where(inside, block, 0.0), done)
        block = jnp.where(here, done, rest)
    return block

def nn(a, b):
    return lax.dot_general(a, b, (((1,), (0,)), ((), ())), precision=HI, preferred_element_type=jnp.float32)

def nt(a, b):
    return lax.dot_general(a, b, (((1,), (1,)), ((), ())), precision=HI, preferred_element_type=jnp.float32)

def factor_solve(h_ref, x_ref, n):
    blocks = n // NB

    def step(k, carry):
        at = pl.ds(pl.multiple_of(k * NB, NB), NB)
        inv = invert_block(h_ref[at, at])
        for kk in range(blocks):
            @pl.when(k == kk)
            def _(kk=kk):
                kc = slice(kk * NB, (kk + 1) * NB)
                s = (kk + 1) * NB
                below = h_ref[s:n + 8, kc]
                w = nn(below, inv)
                c = s
                while c < n:
                    wd = min(256, n - c)
                    h_ref[c:n + 8, c:c + wd] -= nt(w[c - s:, :], below[c - s:c - s + wd, :])
                    c += wd
                h_ref[s:n + 8, kc] = w
        return carry

    lax.fori_loop(0, blocks, step, 0)
    for k in reversed(range(blocks)):
        kc = slice(k * NB, (k + 1) * NB)
        s = (k + 1) * NB
        y = h_ref[n:n + 8, kc]
        if s < n:
            y = y - nn(x_ref[:, s:], h_ref[s:n, kc])
        x_ref[:, kc] = y


def solve_kernel(total, parts, where_ref, *refs):
    halves, (g_ref, x_ref, s_ref, h_ref) = refs[: 2 * len(parts)], refs[2 * len(parts):]
    n = s_ref.shape[1]

    def place(j, carry):
        outer, inner = j >> 2, j & 3
        for i, (low, high, order) in enumerate(parts):
            at = [0, 0]
            at[order[0]] = (outer + where_ref[order[0]]) & 3
            at[order[1]] = (inner + where_ref[order[1]]) & 3
            for partner in range(2):
                src = halves[2 * i + partner]
                core = where_ref[3] ^ partner
                for last in range(4):
                    to = (((core * 4 + at[0]) * 4 + at[1]) * 4 + ((last + where_ref[2]) & 3)) * 16
                    to = pl.ds(pl.multiple_of(to, 16), 16)
                    for c in range(high - low):
                        start = pl.multiple_of((j * 4 + last) * ((high - low) * 16) + c * 16, 16)
                        s_ref[to, (low + c) * 128:(low + c + 1) * 128] = src[pl.ds(start, 16), :]
        return carry

    lax.fori_loop(0, 16, place, 0)
    for c in range(0, n, 256):
        gram = lax.dot_general(
            s_ref[:, c:], s_ref[:, c:c + 256], (((0,), (0,)), ((), ())), preferred_element_type=jnp.float32
        )
        r = lax.broadcasted_iota(jnp.int32, gram.shape, 0)
        q = lax.broadcasted_iota(jnp.int32, gram.shape, 1)
        h_ref[c:n, c:c + 256] = gram / total + jnp.where(r == q, ridge, 0.0)
    h_ref[n:n + 8, :] = jnp.broadcast_to(g_ref[...], (8, n))
    factor_solve(h_ref, x_ref, n)


def solve(pieces, gradient, where, total):
    n = gradient.shape[0]
    rows = 2 * 64 * 16
    vmem = pl.BlockSpec(memory_space=pltpu.VMEM)
    return pl.pallas_call(
        functools.partial(solve_kernel, total, PARTS),
        out_shape=jax.ShapeDtypeStruct((8, n), jnp.float32),
        in_specs=[pl.BlockSpec(memory_space=pltpu.SMEM)] + [vmem] * (len(pieces) + 1),
        out_specs=vmem,
        scratch_shapes=[pltpu.VMEM((rows, n), jnp.bfloat16), pltpu.VMEM((n + 8, n), jnp.float32)],
        compiler_params=pltpu.CompilerParams(vmem_limit_bytes=48 << 20),
        name="solve",
    )(where, *pieces, gradient[None, :])[0]


def reduce_over_devices(mine, other, grad):
    blocks, g = list(mine), grad
    count = grad.shape[0]

    def exchange(x, axis, k, with_grad):
        flat = x.reshape(-1, x.shape[-1])
        if not with_grad:
            return shift(flat, axis, k).reshape(x.shape), g
        got = shift(jnp.concatenate([flat, g], 0), axis, k)
        return got[:-count].reshape(x.shape), got[-count:]

    for i in range(len(PARTS)):
        got, got_g = exchange(other[i], 3, 1, i == 1)
        blocks[i] = blocks[i] + got
    g = g + got_g
    for stage in range(2):
        for i, (_, _, order) in enumerate(PARTS):
            axis = order[stage]
            pos = axis if stage == 0 else 0
            terms, terms_g = [lax.index_in_dim(blocks[i], 0, pos, False)], [g]
            for k in (1, 2, 3):
                got, got_g = exchange(lax.index_in_dim(blocks[i], k, pos, False), axis, k, i == 1)
                terms.append(got)
                terms_g.append(got_g)
            blocks[i] = sum_of_four(terms)
        g = sum_of_four(terms_g)
    both = jnp.concatenate(blocks, 1)
    terms, terms_g = [both], [g]
    for k in (1, 2, 3):
        got, got_g = exchange(both, 2, k, True)
        terms.append(jnp.roll(got, -k, 0))
        terms_g.append(got_g)
    both = sum_of_four(terms).astype(jnp.bfloat16)
    g = sum_of_four(terms_g)
    half = both.shape[1] // 2
    blocks = [both[:, :half].reshape(-1, 128), both[:, half:].reshape(-1, 128)]
    for stage in (1, 0):
        for i, (_, _, order) in enumerate(PARTS):
            got = [blocks[i]] + [shift(blocks[i], order[stage], k) for k in (3, 2, 1)]
            blocks[i] = jnp.concatenate(got, 0)
    pieces = []
    for b in blocks:
        pieces += [b, shift(b, 3, 1)]
    return pieces, g


def sum_over_devices(x):
    x = x + shift(x, 3, 1)
    for axis in range(3):
        x = sum_of_four([x] + [shift(x, axis, k) for k in (1, 2, 3)])
    return x


def front_kernel(where_ref, at_ref, coef_ref, w_ref, label_ref, sign_ref, x_ref,
                 margin_ref, grad_ref, a_ref, b_ref, had_ref, mix_ref):
    step = pl.program_id(0)
    sub_blocks = x_ref.shape[0] // 256
    blocks = 16 // sub_blocks

    @pl.when(step == 0)
    def _():
        i = lax.broadcasted_iota(jnp.int32, (256, 256), 0)
        j = lax.broadcasted_iota(jnp.int32, (256, 256), 1)
        v = i & j
        v = v ^ (v >> 4)
        v = v ^ (v >> 2)
        v = (v ^ (v >> 1)) & 1
        had_ref[...] = jnp.where(v == 0, 1.0, -1.0).astype(jnp.bfloat16)
        grad_ref[...] = jnp.zeros_like(grad_ref)

    @pl.when(step < blocks)
    def _():
        low = jnp.broadcast_to(w_ref[...], (8, w_ref.shape[1])).astype(jnp.bfloat16)
        for sb in range(sub_blocks):
            rows = slice(sb * 256, (sb + 1) * 256)
            x = x_ref[rows, :]
            margin = lax.dot_general(low, x, (((1,), (1,)), ((), ())), preferred_element_type=jnp.float32)
            prob = jax.nn.sigmoid(margin)
            target = label_ref[:, rows].astype(jnp.float32)
            misfit = (prob - target).astype(jnp.bfloat16)
            spread = prob * (1.0 - prob)
            factor = jnp.where(spread > 0.0, jnp.sqrt(spread), 0.0)
            factor = (1.0 - 2.0 * sign_ref[:, rows].astype(jnp.float32)) * factor
            margin_ref[:, rows] = margin[:1, :]
            grad_ref[...] += jnp.dot(misfit, x, preferred_element_type=jnp.float32)
            column = jnp.broadcast_to(factor[:1, :], (128, 256)).T
            for c in range(8):
                cols = slice(c * 128, (c + 1) * 128)
                scaled = (x[:, cols].astype(jnp.float32) * column).astype(jnp.bfloat16)
                first = jnp.dot(had_ref[...], scaled, preferred_element_type=jnp.float32)
                at = (step * sub_blocks + sb) * 32
                mix_ref[pl.ds(at, 32), c * 8:(c + 1) * 8, :] = first.reshape(32, 8, 128)

    @pl.when(step == blocks)
    def _():
        def butterflies(t, carry):
            for c in range(8):
                cols = slice(c * 8, (c + 1) * 8)
                v = [mix_ref[t + 32 * k, cols, :] for k in range(16)]
                for bit in (1, 2, 4, 8):
                    v = [v[k] + v[k ^ bit] if not k & bit else v[k ^ bit] - v[k] for k in range(16)]
                for k in range(16):
                    mix_ref[t + 32 * k, cols, :] = v[k]
            return carry

        lax.fori_loop(0, 32, butterflies, 0)

    @pl.when(step >= blocks)
    def _():
        flat = mix_ref.reshape(512 * 64, 128)
        here = a_ref.shape[0]

        def pick(i, carry):
            p = (step - blocks) * here + i
            core = (p >> 6) ^ where_ref[3]
            chip = 0
            for axis, bits in ((0, 4), (1, 2), (2, 0)):
                chip = chip * 4 + (((p >> bits) + where_ref[axis]) & 3)
            base = (chip * 2 + core) * 16
            for s in range(16):
                at = at_ref[base + s]
                coef = coef_ref[base + s]
                for out, start, count in ((a_ref, 0, 4), (b_ref, 32, 4)):
                    got = flat[pl.ds(at + start, count, stride=8), :]
                    out[i, pl.ds(s, count, stride=16), :] = got * coef
            return carry

        lax.fori_loop(0, here, pick, 0)


def front(design, weights, labels, signs, rows, coefs, where):
    rows_here, width = design.shape
    block = 512
    smem = pl.BlockSpec(memory_space=pltpu.SMEM)
    whole = lambda *shape: pl.BlockSpec(shape, lambda i: (0,) * len(shape))
    picked = [(128, 64, 128), (128, 64, 128)]
    blocks, outs = rows_here // block, 4
    at = (rows >> 3) * 64 + (rows & 7)
    part = lambda s: pl.BlockSpec((s[0] // outs, *s[1:]), lambda i: (jnp.maximum(i - blocks, 0), 0, 0))
    held = lambda i: jnp.minimum(i, blocks - 1)
    return pl.pallas_call(
        front_kernel,
        grid=(blocks + outs,),
        out_shape=[
            jax.ShapeDtypeStruct((1, rows_here), jnp.float32),
            jax.ShapeDtypeStruct((8, width), jnp.float32),
        ] + [jax.ShapeDtypeStruct(s, jnp.float32) for s in picked],
        in_specs=[
            smem, smem, smem,
            whole(1, width),
            pl.BlockSpec((1, block), lambda i: (0, held(i))),
            pl.BlockSpec((1, block), lambda i: (0, held(i))),
            pl.BlockSpec((block, width), lambda i: (held(i), 0)),
        ],
        out_specs=[pl.BlockSpec((1, block), lambda i: (0, held(i))), whole(8, width)] + [part(s) for s in picked],
        scratch_shapes=[pltpu.VMEM((256, 256), jnp.bfloat16), pltpu.VMEM((512, 64, 128), jnp.float32)],
        compiler_params=pltpu.CompilerParams(vmem_limit_bytes=48 << 20),
        name="front",
    )(where, at, coefs, weights[None, :], labels[None, :], signs[None, :], design)


def body(design, weights, labels, signs, sample_rows):
    rows_here, width = design.shape
    device_count = lax.axis_size(ROWS)
    device_index = lax.axis_index(ROWS)
    where = jnp.stack([lax.axis_index(a) for a in ROWS])
    total_rows = rows_here * device_count
    norm_factor = 1.0 / jnp.sqrt(jnp.float32(sample_rows.shape[0]))
    parity = (sample_rows // rows_here) & device_index
    for bits in (4, 2, 1):
        parity = parity ^ (parity >> bits)
    coefs = (1 - 2 * (parity & 1)).astype(jnp.float32) * norm_factor
    margins, grad_part, *picked = front(
        design, weights, labels, signs, sample_rows % rows_here, coefs, where
    )
    picked = [p.reshape(2, 4, 4, 4, -1, 128) for p in picked]
    mine = [p[0] for p in picked]
    other = [p[1] for p in picked]
    pieces, grad = reduce_over_devices(mine, other, grad_part[0].reshape(8, 128))
    gradient = grad.reshape(-1) / total_rows + ridge * weights
    newton_step = solve(pieces, gradient, where, float(total_rows))
    along = jnp.dot(design, newton_step.astype(jnp.bfloat16), preferred_element_type=jnp.float32)
    lengths = jnp.array([1.0, 0.5, 0.25, 0.125], jnp.float32)
    margins = margins[0]
    target = labels.astype(jnp.float32)
    trial = margins[None, :] - lengths[:, None] * along[None, :]
    row_loss = jnp.logaddexp(0.0, trial) - target[None, :] * trial
    loss_total = sum_over_devices(jnp.sum(row_loss, axis=1))
    moved = weights[None, :] - lengths[:, None] * newton_step[None, :]
    losses = loss_total / total_rows + 0.5 * ridge * jnp.sum(moved * moved, axis=1)
    return (gradient, newton_step, losses)


def solution(mesh):
    torus = Mesh(mesh.devices.reshape(4, 4, 4, 2), ROWS)
    in_specs = (P(ROWS, None), P(), P(ROWS), P(ROWS), P())
    out_specs = (P(), P(), P())
    return jax.shard_map(body, mesh=torus, in_specs=in_specs, out_specs=out_specs, check_vma=False)
```

```python
import functools

import jax
import jax.numpy as jnp
from jax import lax
from jax.experimental import pallas as pl
from jax.experimental.pallas import tpu as pltpu
from jax.sharding import Mesh
from jax.sharding import PartitionSpec as P

ROWS = ("rows_0", "rows_1", "rows_2", "rows_3")

ridge = 0.05

PARTS = ((0, 4, (0, 1)), (4, 8, (1, 0)))


def shift(x, axis, k):
    size = 2 if axis == 3 else 4
    return lax.ppermute(x, ROWS[axis], [(i, (i + k) % size) for i in range(size)])


def sum_of_four(x):
    return (x[0] + x[2]) + (x[1] + x[3])


NB = 128

def row_of(x, j):
    return jnp.broadcast_to(x[j:j + 1, :], x.shape)

def col_of(x, j):
    return jnp.broadcast_to(x[:, j:j + 1], x.shape)

def invert_block(block):
    lane = lax.broadcasted_iota(jnp.int32, (8, NB), 1)
    sub = lax.broadcasted_iota(jnp.int32, (8, NB), 0)
    lanes = lax.broadcasted_iota(jnp.int32, (NB, NB), 1)
    rows = lax.broadcasted_iota(jnp.int32, (NB, NB), 0)
    real = lane < NB
    for p in range(4):
        tiles = [block[32 * p + 8 * t:32 * p + 8 * t + 8, :] for t in range(4)]
        for q in range(2):
            base = 32 * p + 16 * q
            inside = (lane >= base) & (lane < base + 16)
            mine, others = (2 * q, 2 * q + 1), (2 - 2 * q, 3 - 2 * q)
            own = [[jnp.where(real, col_of(tiles[t], base + j), 0.0) for t in mine] for j in range(16)]
            cols = {i: [col_of(tiles[i], base + j) for j in range(16)] for i in others}
            panel = [
                jnp.where(inside, jnp.where(lane - base == sub + 8 * h, 1.0, 0.0), tiles[mine[h]]) for h in range(2)
            ]
            for j in range(0, 16, 2):
                half, r = j // 8, j % 8
                first, second = own[j], own[j + 1]
                a, b = row_of(first[half], r), row_of(second[half], r)
                c, d = row_of(first[half], r + 1), row_of(second[half], r + 1)
                inv = 1.0 / (a * d - b * c)
                a, b, c, d = d * inv, b * inv, c * inv, a * inv

                def eliminate(x):
                    top, low = row_of(x[half], r), row_of(x[half], r + 1)
                    top, low = a * top - b * low, d * low - c * top
                    out = [x[h] - first[h] * top - second[h] * low for h in range(2)]
                    out[half] = jnp.where(sub == r, top, jnp.where(sub == r + 1, low, out[half]))
                    return out

                for k in range(j + 2, 16):
                    own[k] = eliminate(own[k])
                panel = eliminate(panel)
            lines = [row_of(panel[j // 8], j % 8) for j in range(16)]
            for i in others:
                t = jnp.where(inside, 0.0, tiles[i])
                for j in range(16):
                    t = t - cols[i][j] * lines[j]
                tiles[i] = t
            tiles[mine[0]], tiles[mine[1]] = panel
        here = (rows >= 32 * p) & (rows < 32 * p + 32)
        inside = (lanes >= 32 * p) & (lanes < 32 * p + 32)
        done = jnp.concatenate([block[:32 * p, :]] * (p > 0) + tiles + [block[32 * p + 32:, :]] * (p < 3), 0)
        rest = jnp.where(inside, 0.0, block) - jnp.dot(
            left(block[:, 32 * p:32 * p + 32]), right(jnp.concatenate(tiles, 0), 0), preferred_element_type=jnp.float32
        )
        block = jnp.where(here, done, rest)
    return block

def thirds(x):
    first = x.astype(jnp.bfloat16).astype(jnp.float32)
    rest = x - first
    second = rest.astype(jnp.bfloat16).astype(jnp.float32)
    return first, second, rest - second


def left(x, axis=1):
    p, q, r = thirds(x)
    return jnp.concatenate([p, q, p, r, p, q], axis).astype(jnp.bfloat16)


def right(x, axis):
    p, q, r = thirds(x)
    return jnp.concatenate([q, q, r, p, p, p], axis).astype(jnp.bfloat16)


def nn(a, b):
    return jnp.dot(left(a), right(b, 0), preferred_element_type=jnp.float32)


def nt(a, b):
    return lax.dot_general(a, b, (((1,), (1,)), ((), ())), preferred_element_type=jnp.float32)


def factor_solve(h_ref, x_ref, n):
    blocks = n // NB

    def step(k, carry):
        at = pl.ds(pl.multiple_of(k * NB, NB), NB)
        inv = invert_block(h_ref[at, at])
        for kk in range(blocks):
            @pl.when(k == kk)
            def _(kk=kk):
                kc = slice(kk * NB, (kk + 1) * NB)
                s = (kk + 1) * NB
                below = h_ref[s:n + 8, kc]
                w = nn(below, inv)
                wide, tall = left(w), right(below, 1)
                c = s
                while c < n:
                    wd = min(256, n - c)
                    h_ref[c:n + 8, c:c + wd] -= nt(wide[c - s:, :], tall[c - s:c - s + wd, :])
                    c += wd
                h_ref[s:n + 8, kc] = w
        return carry

    lax.fori_loop(0, blocks, step, 0)
    for k in reversed(range(blocks)):
        kc = slice(k * NB, (k + 1) * NB)
        s = (k + 1) * NB
        y = h_ref[n:n + 8, kc]
        if s < n:
            y = y - nn(x_ref[:, s:], h_ref[s:n, kc])
        x_ref[:, kc] = y


def solve_kernel(total, parts, where_ref, *refs):
    halves, (g_ref, x_ref, s_ref, h_ref) = refs[: 2 * len(parts)], refs[2 * len(parts):]
    n = s_ref.shape[1]

    def place(j, carry):
        outer, inner = j >> 2, j & 3
        for i, (low, high, order) in enumerate(parts):
            at = [0, 0]
            at[order[0]] = (outer + where_ref[order[0]]) & 3
            at[order[1]] = (inner + where_ref[order[1]]) & 3
            for partner in range(2):
                src = halves[2 * i + partner]
                core = where_ref[3] ^ partner
                for last in range(4):
                    to = (((core * 4 + at[0]) * 4 + at[1]) * 4 + ((last + where_ref[2]) & 3)) * 16
                    to = pl.ds(pl.multiple_of(to, 16), 16)
                    for c in range(high - low):
                        start = pl.multiple_of((j * 4 + last) * ((high - low) * 16) + c * 16, 16)
                        s_ref[to, (low + c) * 128:(low + c + 1) * 128] = src[pl.ds(start, 16), :]
        return carry

    lax.fori_loop(0, 16, place, 0)
    for c in range(0, n, 256):
        gram = lax.dot_general(
            s_ref[:, c:], s_ref[:, c:c + 256], (((0,), (0,)), ((), ())), preferred_element_type=jnp.float32
        )
        r = lax.broadcasted_iota(jnp.int32, gram.shape, 0)
        q = lax.broadcasted_iota(jnp.int32, gram.shape, 1)
        h_ref[c:n, c:c + 256] = gram / total + jnp.where(r == q, ridge, 0.0)
    h_ref[n:n + 8, :] = jnp.broadcast_to(g_ref[...], (8, n))
    factor_solve(h_ref, x_ref, n)


def solve(pieces, gradient, where, total):
    n = gradient.shape[0]
    rows = 2 * 64 * 16
    vmem = pl.BlockSpec(memory_space=pltpu.VMEM)
    return pl.pallas_call(
        functools.partial(solve_kernel, total, PARTS),
        out_shape=jax.ShapeDtypeStruct((8, n), jnp.float32),
        in_specs=[pl.BlockSpec(memory_space=pltpu.SMEM)] + [vmem] * (len(pieces) + 1),
        out_specs=vmem,
        scratch_shapes=[pltpu.VMEM((rows, n), jnp.bfloat16), pltpu.VMEM((n + 8, n), jnp.float32)],
        compiler_params=pltpu.CompilerParams(vmem_limit_bytes=48 << 20),
        name="solve",
    )(where, *pieces, gradient[None, :])[0]


def reduce_over_devices(mine, other, grad):
    blocks, g = list(mine), grad
    count = grad.shape[0]

    def exchange(x, axis, k, with_grad):
        flat = x.reshape(-1, x.shape[-1])
        if not with_grad:
            return shift(flat, axis, k).reshape(x.shape), g
        got = shift(jnp.concatenate([flat, g], 0), axis, k)
        return got[:-count].reshape(x.shape), got[-count:]

    for i in range(len(PARTS)):
        blocks[i] = blocks[i] + exchange(other[i], 3, 1, False)[0]
    g = g + shift(g, 3, 1)
    for i, (_, _, order) in enumerate(PARTS):
        axis = order[0]
        b = [lax.index_in_dim(blocks[i], k, axis, False) for k in range(4)]
        up, up_g = exchange(b[2][:2], axis, 1, i == 1)
        down, down_g = exchange(b[2][2:], axis, 3, i == 1)
        near = jnp.concatenate([b[1][:2] + up, b[1][2:]], 0)
        far = jnp.concatenate([b[3][:2], b[3][2:] + down], 0)
        if i == 1:
            flat = shift(jnp.concatenate([near.reshape(-1, 128), up_g], 0), axis, 1)
            near, across_g = flat[:-count].reshape(near.shape), flat[-count:]
        else:
            near = shift(near.reshape(-1, 128), axis, 1).reshape(near.shape)
        far = shift(far.reshape(-1, 128), axis, 3).reshape(far.shape)
        blocks[i] = b[0] + (near + far)
    g = (g + across_g) + (up_g + down_g)
    for i, (_, _, order) in enumerate(PARTS):
        terms, terms_g = [blocks[i][0]], [g]
        for k in (1, 2, 3):
            got, got_g = exchange(blocks[i][k], order[1], k, i == 1)
            terms.append(got)
            terms_g.append(got_g)
        blocks[i] = sum_of_four(terms)
    g = sum_of_four(terms_g)
    both = jnp.concatenate(blocks, 1)
    terms, terms_g = [both], [g]
    for k in (1, 2, 3):
        got, got_g = exchange(both, 2, k, True)
        terms.append(jnp.roll(got, -k, 0))
        terms_g.append(got_g)
    both = sum_of_four(terms).astype(jnp.bfloat16)
    g = sum_of_four(terms_g)
    half = both.shape[1] // 2
    blocks = [both[:, :half].reshape(-1, 128), both[:, half:].reshape(-1, 128)]
    for stage in (1, 0):
        for i, (_, _, order) in enumerate(PARTS):
            got = [blocks[i]] + [shift(blocks[i], order[stage], k) for k in (3, 2, 1)]
            blocks[i] = jnp.concatenate(got, 0)
    pieces = []
    for b in blocks:
        pieces += [b, shift(b, 3, 1)]
    return pieces, g


def sum_over_devices(x):
    x = x + shift(x, 3, 1)
    for axis in range(3):
        x = sum_of_four([x] + [shift(x, axis, k) for k in (1, 2, 3)])
    return x


def front_kernel(where_ref, at_ref, coef_ref, w_ref, label_ref, sign_ref, x_ref,
                 margin_ref, grad_ref, other_a_ref, other_b_ref, mine_a_ref, mine_b_ref, had_ref, mix_ref):
    step = pl.program_id(0)
    sub_blocks = x_ref.shape[0] // 256
    blocks = 16 // sub_blocks

    @pl.when(step == 0)
    def _():
        i = lax.broadcasted_iota(jnp.int32, (256, 256), 0)
        j = lax.broadcasted_iota(jnp.int32, (256, 256), 1)
        v = i & j
        v = v ^ (v >> 4)
        v = v ^ (v >> 2)
        v = (v ^ (v >> 1)) & 1
        had_ref[...] = jnp.where(v == 0, 1.0, -1.0).astype(jnp.bfloat16)
        grad_ref[...] = jnp.zeros_like(grad_ref)

    @pl.when(step < blocks)
    def _():
        low = jnp.broadcast_to(w_ref[...], (8, w_ref.shape[1])).astype(jnp.bfloat16)
        x = x_ref[...]
        margin = lax.dot_general(low, x, (((1,), (1,)), ((), ())), preferred_element_type=jnp.float32)
        prob = jax.nn.sigmoid(margin)
        target = label_ref[...].astype(jnp.float32)
        misfit = (prob - target).astype(jnp.bfloat16)
        spread = prob * (1.0 - prob)
        factor = jnp.where(spread > 0.0, jnp.sqrt(spread), 0.0)
        factor = (1.0 - 2.0 * sign_ref[...].astype(jnp.float32)) * factor
        margin_ref[...] = margin[:1, :]
        columns = [
            jnp.broadcast_to(factor[:1, sb * 256:(sb + 1) * 256], (128, 256)).T for sb in range(sub_blocks)
        ]
        for sb in range(sub_blocks):
            rows = slice(sb * 256, (sb + 1) * 256)
            for c in range(8):
                cols = slice(c * 128, (c + 1) * 128)
                scaled = (x_ref[rows, cols].astype(jnp.float32) * columns[sb]).astype(jnp.bfloat16)
                first = jnp.dot(had_ref[...], scaled, preferred_element_type=jnp.float32)
                at = (step * sub_blocks + sb) * 32
                mix_ref[pl.ds(at, 32), c * 8:(c + 1) * 8, :] = first.reshape(32, 8, 128)
        grad_ref[...] += jnp.dot(misfit, x_ref[...], preferred_element_type=jnp.float32)

    @pl.when(step == blocks)
    def _():
        def butterflies(t, carry):
            for c in range(8):
                cols = slice(c * 8, (c + 1) * 8)
                v = [mix_ref[t + 32 * k, cols, :] for k in range(16)]
                for bit in (1, 2, 4, 8):
                    v = [v[k] + v[k ^ bit] if not k & bit else v[k ^ bit] - v[k] for k in range(16)]
                for k in range(16):
                    mix_ref[t + 32 * k, cols, :] = v[k]
            return carry

        lax.fori_loop(0, 32, butterflies, 0)

    here = other_a_ref.shape[0]
    stages = 64 // here

    def pick_into(a_ref, b_ref, core, stage):
        flat = mix_ref.reshape(512 * 64, 128)

        def pick(i, carry):
            p = stage * here + i
            chip = 0
            for axis, bits in ((0, 4), (1, 2), (2, 0)):
                chip = chip * 4 + (((p >> bits) + where_ref[axis]) & 3)
            base = (chip * 2 + core) * 16
            for s in range(16):
                at = at_ref[base + s]
                coef = coef_ref[base + s]
                for out, start, count in ((a_ref, 0, 4), (b_ref, 32, 4)):
                    got = flat[pl.ds(at + start, count, stride=8), :]
                    out[i, pl.ds(s, count, stride=16), :] = got * coef
            return carry

        lax.fori_loop(0, here, pick, 0)

    @pl.when((step >= blocks) & (step < blocks + stages))
    def _():
        pick_into(other_a_ref, other_b_ref, 1 - where_ref[3], step - blocks)

    @pl.when(step >= blocks + stages)
    def _():
        pick_into(mine_a_ref, mine_b_ref, where_ref[3], step - blocks - stages)


def front(design, weights, labels, signs, rows, coefs, where):
    rows_here, width = design.shape
    block = 1024
    smem = pl.BlockSpec(memory_space=pltpu.SMEM)
    whole = lambda *shape: pl.BlockSpec(shape, lambda i: (0,) * len(shape))
    picked = [(64, 64, 128)] * 4
    blocks, stages = rows_here // block, 2
    at = (rows >> 3) * 64 + (rows & 7)
    shape = (64 // stages, 64, 128)
    first = pl.BlockSpec(shape, lambda i: (jnp.clip(i - blocks, 0, stages - 1), 0, 0))
    second = pl.BlockSpec(shape, lambda i: (jnp.clip(i - blocks - stages, 0, stages - 1), 0, 0))
    held = lambda i: jnp.minimum(i, blocks - 1)
    return pl.pallas_call(
        front_kernel,
        grid=(blocks + 2 * stages,),
        out_shape=[
            jax.ShapeDtypeStruct((1, rows_here), jnp.float32),
            jax.ShapeDtypeStruct((8, width), jnp.float32),
        ] + [jax.ShapeDtypeStruct(s, jnp.float32) for s in picked],
        in_specs=[
            smem, smem, smem,
            whole(1, width),
            pl.BlockSpec((1, block), lambda i: (0, held(i))),
            pl.BlockSpec((1, block), lambda i: (0, held(i))),
            pl.BlockSpec((block, width), lambda i: (held(i), 0)),
        ],
        out_specs=[pl.BlockSpec((1, block), lambda i: (0, held(i))), whole(8, width)] + [first, first, second, second],
        scratch_shapes=[pltpu.VMEM((256, 256), jnp.bfloat16), pltpu.VMEM((512, 64, 128), jnp.float32)],
        compiler_params=pltpu.CompilerParams(vmem_limit_bytes=48 << 20),
        name="front",
    )(where, at, coefs, weights[None, :], labels[None, :], signs[None, :], design)


def body(design, weights, labels, signs, sample_rows):
    rows_here, width = design.shape
    device_count = lax.axis_size(ROWS)
    device_index = lax.axis_index(ROWS)
    where = jnp.stack([lax.axis_index(a) for a in ROWS])
    total_rows = rows_here * device_count
    norm_factor = 1.0 / jnp.sqrt(jnp.float32(sample_rows.shape[0]))
    parity = (sample_rows // rows_here) & device_index
    for bits in (4, 2, 1):
        parity = parity ^ (parity >> bits)
    coefs = (1 - 2 * (parity & 1)).astype(jnp.float32) * norm_factor
    margins, grad_part, *halves = front(
        design, weights, labels, signs, sample_rows % rows_here, coefs, where
    )
    halves = [h.reshape(4, 4, 4, -1, 128) for h in halves]
    pieces, grad = reduce_over_devices(halves[2:], halves[:2], grad_part[0].reshape(8, 128))
    gradient = grad.reshape(-1) / total_rows + ridge * weights
    newton_step = solve(pieces, gradient, where, float(total_rows))
    along = jnp.dot(design, newton_step.astype(jnp.bfloat16), preferred_element_type=jnp.float32)
    lengths = jnp.array([1.0, 0.5, 0.25, 0.125], jnp.float32)
    margins = margins[0]
    target = labels.astype(jnp.float32)
    trial = margins[None, :] - lengths[:, None] * along[None, :]
    row_loss = jnp.logaddexp(0.0, trial) - target[None, :] * trial
    loss_total = sum_over_devices(jnp.sum(row_loss, axis=1))
    moved = weights[None, :] - lengths[:, None] * newton_step[None, :]
    losses = loss_total / total_rows + 0.5 * ridge * jnp.sum(moved * moved, axis=1)
    return (gradient, newton_step, losses)


def solution(mesh):
    torus = Mesh(mesh.devices.reshape(4, 4, 4, 2), ROWS)
    in_specs = (P(ROWS, None), P(), P(ROWS), P(ROWS), P())
    out_specs = (P(), P(), P())
    return jax.shard_map(body, mesh=torus, in_specs=in_specs, out_specs=out_specs, check_vma=False)
```

```python
import functools

import jax
import jax.numpy as jnp
from jax import lax
from jax.experimental import pallas as pl
from jax.experimental.pallas import tpu as pltpu
from jax.sharding import Mesh
from jax.sharding import PartitionSpec as P

ROWS = ("rows_0", "rows_1", "rows_2", "rows_3")

ridge = 0.05

PARTS = ((0, 4, (0, 1)), (4, 8, (1, 0)))


def shift(x, axis, k):
    size = 2 if axis == 3 else 4
    return lax.ppermute(x, ROWS[axis], [(i, (i + k) % size) for i in range(size)])


def sum_of_four(x):
    return (x[0] + x[2]) + (x[1] + x[3])


NB = 128

def row_of(x, j):
    return jnp.broadcast_to(x[j:j + 1, :], x.shape)

def col_of(x, j):
    return jnp.broadcast_to(x[:, j:j + 1], x.shape)

def invert_block(block):
    lane = lax.broadcasted_iota(jnp.int32, (8, NB), 1)
    sub = lax.broadcasted_iota(jnp.int32, (8, NB), 0)
    lanes = lax.broadcasted_iota(jnp.int32, (64, NB), 1)
    real = lane < NB
    halves = [block[:64, :], block[64:, :]]
    for p in range(2):
        tiles = [halves[p][8 * t:8 * t + 8, :] for t in range(8)]
        for q in range(4):
            base = 64 * p + 16 * q
            inside = (lane >= base) & (lane < base + 16)
            mine = (2 * q, 2 * q + 1)
            others = [(2 * q + 2 + t) % 8 for t in range(6)]
            own = [[jnp.where(real, col_of(tiles[t], base + j), 0.0) for t in mine] for j in range(16)]
            cols = {i: [col_of(tiles[i], base + j) for j in range(16)] for i in others}
            panel = [
                jnp.where(inside, jnp.where(lane - base == sub + 8 * h, 1.0, 0.0), tiles[mine[h]]) for h in range(2)
            ]
            for j in range(0, 16, 2):
                half, r = j // 8, j % 8
                first, second = own[j], own[j + 1]
                a, b = row_of(first[half], r), row_of(second[half], r)
                c, d = row_of(first[half], r + 1), row_of(second[half], r + 1)
                inv = 1.0 / (a * d - b * c)
                a, b, c, d = d * inv, b * inv, c * inv, a * inv

                def eliminate(x):
                    top, low = row_of(x[half], r), row_of(x[half], r + 1)
                    top, low = a * top - b * low, d * low - c * top
                    out = [x[h] - first[h] * top - second[h] * low for h in range(2)]
                    out[half] = jnp.where(sub == r, top, jnp.where(sub == r + 1, low, out[half]))
                    return out

                for k in range(j + 2, 16):
                    own[k] = eliminate(own[k])
                panel = eliminate(panel)
            lines = [row_of(panel[j // 8], j % 8) for j in range(16)]
            for i in others:
                t = jnp.where(inside, 0.0, tiles[i])
                for j in range(16):
                    t = t - cols[i][j] * lines[j]
                tiles[i] = t
            tiles[mine[0]], tiles[mine[1]] = panel
        done, rest = jnp.concatenate(tiles, 0), halves[1 - p]
        here = (lanes >= 64 * p) & (lanes < 64 * p + 64)
        halves[p] = done
        halves[1 - p] = jnp.where(here, 0.0, rest) - nn(rest[:, 64 * p:64 * p + 64], done)
    return jnp.concatenate(halves, 0)


def thirds(x):
    first = x.astype(jnp.bfloat16).astype(jnp.float32)
    rest = x - first
    second = rest.astype(jnp.bfloat16).astype(jnp.float32)
    return first, second, rest - second


def left(x, axis=1):
    p, q, r = thirds(x)
    return jnp.concatenate([p, q, p, r, p, q], axis).astype(jnp.bfloat16)


def right(x, axis):
    p, q, r = thirds(x)
    return jnp.concatenate([q, q, r, p, p, p], axis).astype(jnp.bfloat16)


def nn(a, b):
    return jnp.dot(left(a), right(b, 0), preferred_element_type=jnp.float32)


def nt(a, b):
    return lax.dot_general(a, b, (((1,), (1,)), ((), ())), preferred_element_type=jnp.float32)


def factor_solve(h_ref, x_ref, n):
    blocks = n // NB

    def step(k, carry):
        at = pl.ds(pl.multiple_of(k * NB, NB), NB)
        inv = invert_block(h_ref[at, at])
        for kk in range(blocks):
            @pl.when(k == kk)
            def _(kk=kk):
                kc = slice(kk * NB, (kk + 1) * NB)
                s = (kk + 1) * NB
                below = h_ref[s:n + 8, kc]
                w = nn(below, inv)
                wide, tall = left(w), right(below, 1)
                c = s
                while c < n:
                    wd = min(256, n - c)
                    h_ref[c:n + 8, c:c + wd] -= nt(wide[c - s:, :], tall[c - s:c - s + wd, :])
                    c += wd
                h_ref[s:n + 8, kc] = w
        return carry

    lax.fori_loop(0, blocks, step, 0)
    for k in reversed(range(blocks)):
        kc = slice(k * NB, (k + 1) * NB)
        s = (k + 1) * NB
        y = h_ref[n:n + 8, kc]
        if s < n:
            y = y - nn(x_ref[:, s:], h_ref[s:n, kc])
        x_ref[:, kc] = y


def solve_kernel(total, parts, where_ref, *refs):
    halves, (g_ref, x_ref, s_ref, h_ref) = refs[: 2 * len(parts)], refs[2 * len(parts):]
    n = s_ref.shape[1]

    def place(j, carry):
        outer, inner = j >> 2, j & 3
        for i, (low, high, order) in enumerate(parts):
            at = [0, 0]
            at[order[0]] = (outer + where_ref[order[0]]) & 3
            at[order[1]] = (inner + where_ref[order[1]]) & 3
            for partner in range(2):
                src = halves[2 * i + partner]
                core = where_ref[3] ^ partner
                for last in range(4):
                    to = (((core * 4 + at[0]) * 4 + at[1]) * 4 + ((last + where_ref[2]) & 3)) * 16
                    to = pl.ds(pl.multiple_of(to, 16), 16)
                    for c in range(high - low):
                        start = pl.multiple_of((j * 4 + last) * ((high - low) * 16) + c * 16, 16)
                        s_ref[to, (low + c) * 128:(low + c + 1) * 128] = src[pl.ds(start, 16), :]
        return carry

    lax.fori_loop(0, 16, place, 0)
    for c in range(0, n, 256):
        gram = lax.dot_general(
            s_ref[:, c:], s_ref[:, c:c + 256], (((0,), (0,)), ((), ())), preferred_element_type=jnp.float32
        )
        r = lax.broadcasted_iota(jnp.int32, gram.shape, 0)
        q = lax.broadcasted_iota(jnp.int32, gram.shape, 1)
        h_ref[c:n, c:c + 256] = gram / total + jnp.where(r == q, ridge, 0.0)
    h_ref[n:n + 8, :] = jnp.broadcast_to(g_ref[...], (8, n))
    factor_solve(h_ref, x_ref, n)


def solve(pieces, gradient, where, total):
    n = gradient.shape[0]
    rows = 2 * 64 * 16
    vmem = pl.BlockSpec(memory_space=pltpu.VMEM)
    return pl.pallas_call(
        functools.partial(solve_kernel, total, PARTS),
        out_shape=jax.ShapeDtypeStruct((8, n), jnp.float32),
        in_specs=[pl.BlockSpec(memory_space=pltpu.SMEM)] + [vmem] * (len(pieces) + 1),
        out_specs=vmem,
        scratch_shapes=[pltpu.VMEM((rows, n), jnp.bfloat16), pltpu.VMEM((n + 8, n), jnp.float32)],
        compiler_params=pltpu.CompilerParams(vmem_limit_bytes=48 << 20),
        name="solve",
    )(where, *pieces, gradient[None, :])[0]


def reduce_over_devices(mine, other, grad):
    blocks, g = list(mine), grad
    count = grad.shape[0]

    def exchange(x, axis, k, with_grad):
        flat = x.reshape(-1, x.shape[-1])
        if not with_grad:
            return shift(flat, axis, k).reshape(x.shape), g
        got = shift(jnp.concatenate([flat, g], 0), axis, k)
        return got[:-count].reshape(x.shape), got[-count:]

    for i in range(len(PARTS)):
        blocks[i] = blocks[i] + exchange(other[i], 3, 1, False)[0]
    g = g + shift(g, 3, 1)
    for i, (_, _, order) in enumerate(PARTS):
        axis = order[0]
        b = [lax.index_in_dim(blocks[i], k, axis, False) for k in range(4)]
        up, up_g = exchange(b[2][:2], axis, 1, i == 1)
        down, down_g = exchange(b[2][2:], axis, 3, i == 1)
        near = jnp.concatenate([b[1][:2] + up, b[1][2:]], 0)
        far = jnp.concatenate([b[3][:2], b[3][2:] + down], 0)
        if i == 1:
            flat = shift(jnp.concatenate([near.reshape(-1, 128), up_g], 0), axis, 1)
            near, across_g = flat[:-count].reshape(near.shape), flat[-count:]
        else:
            near = shift(near.reshape(-1, 128), axis, 1).reshape(near.shape)
        far = shift(far.reshape(-1, 128), axis, 3).reshape(far.shape)
        blocks[i] = b[0] + (near + far)
    g = (g + across_g) + (up_g + down_g)
    for i, (_, _, order) in enumerate(PARTS):
        terms, terms_g = [blocks[i][0]], [g]
        for k in (1, 2, 3):
            got, got_g = exchange(blocks[i][k], order[1], k, i == 1)
            terms.append(got)
            terms_g.append(got_g)
        blocks[i] = sum_of_four(terms)
    g = sum_of_four(terms_g)
    both = jnp.concatenate(blocks, 1)
    terms, terms_g = [both], [g]
    for k in (1, 2, 3):
        got, got_g = exchange(both, 2, k, True)
        terms.append(jnp.roll(got, -k, 0))
        terms_g.append(got_g)
    both = sum_of_four(terms).astype(jnp.bfloat16)
    g = sum_of_four(terms_g)
    half = both.shape[1] // 2
    blocks = [both[:, :half].reshape(-1, 128), both[:, half:].reshape(-1, 128)]
    for stage in (1, 0):
        for i, (_, _, order) in enumerate(PARTS):
            got = [blocks[i]] + [shift(blocks[i], order[stage], k) for k in (3, 2, 1)]
            blocks[i] = jnp.concatenate(got, 0)
    pieces = []
    for b in blocks:
        pieces += [b, shift(b, 3, 1)]
    return pieces, g


def small_shift(x, stage, k):
    pairs = []
    for device in range(128):
        unit = (32, 8, 2)[2 - stage if device & 1 else stage]
        at = device // unit % 4
        pairs.append((device, device + ((at + k) % 4 - at) * unit))
    return lax.ppermute(x, ROWS, pairs)


def sum_over_devices(x):
    for stage in range(3):
        x = sum_of_four([x] + [small_shift(x, stage, k) for k in (1, 2, 3)])
    return x + shift(x, 3, 1)


def front_kernel(where_ref, at_ref, coef_ref, w_ref, code_ref, x_ref,
                 margin_ref, grad_ref, other_a_ref, other_b_ref, mine_a_ref, mine_b_ref, had_ref, mix_ref):
    step = pl.program_id(0)
    sub_blocks = x_ref.shape[0] // 256
    blocks = 16 // sub_blocks

    @pl.when(step == 0)
    def _():
        i = lax.broadcasted_iota(jnp.int32, (256, 256), 0)
        j = lax.broadcasted_iota(jnp.int32, (256, 256), 1)
        v = i & j
        v = v ^ (v >> 4)
        v = v ^ (v >> 2)
        v = (v ^ (v >> 1)) & 1
        had_ref[...] = jnp.where(v == 0, 1.0, -1.0).astype(jnp.bfloat16)
        grad_ref[...] = jnp.zeros_like(grad_ref)

    @pl.when(step < blocks)
    def _():
        low = jnp.broadcast_to(w_ref[...], (8, w_ref.shape[1])).astype(jnp.bfloat16)
        x = x_ref[...]
        margin = lax.dot_general(low, x, (((1,), (1,)), ((), ())), preferred_element_type=jnp.float32)
        prob = jax.nn.sigmoid(margin)
        code = code_ref[...]
        target = (code & 1).astype(jnp.float32)
        misfit = (prob - target).astype(jnp.bfloat16)
        spread = prob * (1.0 - prob)
        factor = jnp.where(spread > 0.0, jnp.sqrt(spread), 0.0)
        factor = (1 - (code & 2)).astype(jnp.float32) * factor
        margin_ref[...] = margin[:1, :]
        columns = [
            jnp.broadcast_to(factor[:1, sb * 256:(sb + 1) * 256], (128, 256)).T for sb in range(sub_blocks)
        ]
        for sb in range(sub_blocks):
            rows = slice(sb * 256, (sb + 1) * 256)
            for c in range(8):
                cols = slice(c * 128, (c + 1) * 128)
                scaled = (x_ref[rows, cols].astype(jnp.float32) * columns[sb]).astype(jnp.bfloat16)
                first = jnp.dot(had_ref[...], scaled, preferred_element_type=jnp.float32)
                at = (step * sub_blocks + sb) * 32
                mix_ref[pl.ds(at, 32), c * 8:(c + 1) * 8, :] = first.reshape(32, 8, 128)
        grad_ref[...] += jnp.dot(misfit, x_ref[...], preferred_element_type=jnp.float32)

    @pl.when(step == blocks)
    def _():
        def butterflies(t, carry):
            for c in range(8):
                cols = slice(c * 8, (c + 1) * 8)
                v = [mix_ref[t + 32 * k, cols, :] for k in range(16)]
                for bit in (1, 2, 4, 8):
                    v = [v[k] + v[k ^ bit] if not k & bit else v[k ^ bit] - v[k] for k in range(16)]
                for k in range(16):
                    mix_ref[t + 32 * k, cols, :] = v[k]
            return carry

        lax.fori_loop(0, 32, butterflies, 0)

    here = other_a_ref.shape[0]
    stages = 64 // here

    def pick_into(a_ref, b_ref, core, stage):
        flat = mix_ref.reshape(512 * 64, 128)

        def pick(i, carry):
            p = stage * here + i
            chip = 0
            for axis, bits in ((0, 4), (1, 2), (2, 0)):
                chip = chip * 4 + (((p >> bits) + where_ref[axis]) & 3)
            base = (chip * 2 + core) * 16
            for s in range(16):
                at = at_ref[base + s]
                coef = coef_ref[base + s]
                for out, start, count in ((a_ref, 0, 4), (b_ref, 32, 4)):
                    got = flat[pl.ds(at + start, count, stride=8), :]
                    out[i, pl.ds(s, count, stride=16), :] = got * coef
            return carry

        lax.fori_loop(0, here, pick, 0)

    @pl.when((step >= blocks) & (step < blocks + stages))
    def _():
        pick_into(other_a_ref, other_b_ref, 1 - where_ref[3], step - blocks)

    @pl.when(step >= blocks + stages)
    def _():
        pick_into(mine_a_ref, mine_b_ref, where_ref[3], step - blocks - stages)


def front(design, weights, labels, signs, rows, coefs, where):
    rows_here, width = design.shape
    block = 1024
    smem = pl.BlockSpec(memory_space=pltpu.SMEM)
    whole = lambda *shape: pl.BlockSpec(shape, lambda i: (0,) * len(shape))
    picked = [(64, 64, 128)] * 4
    blocks, stages = rows_here // block, 2
    at = (rows >> 3) * 64 + (rows & 7)
    shape = (64 // stages, 64, 128)
    first = pl.BlockSpec(shape, lambda i: (jnp.clip(i - blocks, 0, stages - 1), 0, 0))
    second = pl.BlockSpec(shape, lambda i: (jnp.clip(i - blocks - stages, 0, stages - 1), 0, 0))
    held = lambda i: jnp.minimum(i, blocks - 1)
    return pl.pallas_call(
        front_kernel,
        grid=(blocks + 2 * stages,),
        out_shape=[
            jax.ShapeDtypeStruct((1, rows_here), jnp.float32),
            jax.ShapeDtypeStruct((8, width), jnp.float32),
        ] + [jax.ShapeDtypeStruct(s, jnp.float32) for s in picked],
        in_specs=[
            smem, smem, smem,
            whole(1, width),
            pl.BlockSpec((1, block), lambda i: (0, held(i))),
            pl.BlockSpec((block, width), lambda i: (held(i), 0)),
        ],
        out_specs=[pl.BlockSpec((1, block), lambda i: (0, held(i))), whole(8, width)] + [first, first, second, second],
        scratch_shapes=[pltpu.VMEM((256, 256), jnp.bfloat16), pltpu.VMEM((512, 64, 128), jnp.float32)],
        compiler_params=pltpu.CompilerParams(vmem_limit_bytes=48 << 20),
        name="front",
    )(where, at, coefs, weights[None, :], (labels + 2 * signs)[None, :], design)


def body(design, weights, labels, signs, sample_rows):
    rows_here, width = design.shape
    device_count = lax.axis_size(ROWS)
    device_index = lax.axis_index(ROWS)
    where = jnp.stack([lax.axis_index(a) for a in ROWS])
    total_rows = rows_here * device_count
    norm_factor = 1.0 / jnp.sqrt(jnp.float32(sample_rows.shape[0]))
    parity = (sample_rows // rows_here) & device_index
    for bits in (4, 2, 1):
        parity = parity ^ (parity >> bits)
    coefs = (1 - 2 * (parity & 1)).astype(jnp.float32) * norm_factor
    margins, grad_part, *halves = front(
        design, weights, labels, signs, sample_rows % rows_here, coefs, where
    )
    halves = [h.reshape(4, 4, 4, -1, 128) for h in halves]
    pieces, grad = reduce_over_devices(halves[2:], halves[:2], grad_part[0].reshape(8, 128))
    gradient = grad.reshape(-1) / total_rows + ridge * weights
    newton_step = solve(pieces, gradient, where, float(total_rows))
    along = jnp.dot(design, newton_step.astype(jnp.bfloat16), preferred_element_type=jnp.float32)
    lengths = jnp.array([1.0, 0.5, 0.25, 0.125], jnp.float32)
    margins = margins[0]
    target = labels.astype(jnp.float32)
    trial = margins[None, :] - lengths[:, None] * along[None, :]
    row_loss = jnp.logaddexp(0.0, trial) - target[None, :] * trial
    loss_total = sum_over_devices(jnp.sum(row_loss, axis=1))
    moved = weights[None, :] - lengths[:, None] * newton_step[None, :]
    losses = loss_total / total_rows + 0.5 * ridge * jnp.sum(moved * moved, axis=1)
    return (gradient, newton_step, losses)


def solution(mesh):
    torus = Mesh(mesh.devices.reshape(4, 4, 4, 2), ROWS)
    in_specs = (P(ROWS, None), P(), P(ROWS), P(ROWS), P())
    out_specs = (P(), P(), P())
    return jax.shard_map(body, mesh=torus, in_specs=in_specs, out_specs=out_specs, check_vma=False)
```

```python
import functools

import jax
import jax.numpy as jnp
from jax import lax
from jax.experimental import pallas as pl
from jax.experimental.pallas import tpu as pltpu
from jax.sharding import Mesh
from jax.sharding import PartitionSpec as P

ROWS = ("rows_0", "rows_1", "rows_2", "rows_3")

ridge = 0.05

PARTS = ((0, 4, (0, 1)), (4, 8, (1, 0)))


def shift(x, axis, k):
    size = 2 if axis == 3 else 4
    return lax.ppermute(x, ROWS[axis], [(i, (i + k) % size) for i in range(size)])


def sum_of_four(x):
    return (x[0] + x[2]) + (x[1] + x[3])


NB = 128

def row_of(x, j):
    return jnp.broadcast_to(x[j:j + 1, :], x.shape)

def col_of(x, j):
    return jnp.broadcast_to(x[:, j:j + 1], x.shape)

def invert_block(block):
    lane = lax.broadcasted_iota(jnp.int32, (8, NB), 1)
    sub = lax.broadcasted_iota(jnp.int32, (8, NB), 0)
    lanes = lax.broadcasted_iota(jnp.int32, (64, NB), 1)
    real = lane < NB
    halves = [block[:64, :], block[64:, :]]
    for p in range(2):
        tiles = [halves[p][8 * t:8 * t + 8, :] for t in range(8)]
        for q in range(4):
            base = 64 * p + 16 * q
            inside = (lane >= base) & (lane < base + 16)
            mine = (2 * q, 2 * q + 1)
            others = [(2 * q + 2 + t) % 8 for t in range(6)]
            own = [[jnp.where(real, col_of(tiles[t], base + j), 0.0) for t in mine] for j in range(16)]
            cols = {i: [col_of(tiles[i], base + j) for j in range(16)] for i in others}
            panel = [
                jnp.where(inside, jnp.where(lane - base == sub + 8 * h, 1.0, 0.0), tiles[mine[h]]) for h in range(2)
            ]
            for j in range(0, 16, 2):
                half, r = j // 8, j % 8
                first, second = own[j], own[j + 1]
                a, b = row_of(first[half], r), row_of(second[half], r)
                c, d = row_of(first[half], r + 1), row_of(second[half], r + 1)
                inv = 1.0 / (a * d - b * c)
                a, b, c, d = d * inv, b * inv, c * inv, a * inv

                def eliminate(x):
                    top, low = row_of(x[half], r), row_of(x[half], r + 1)
                    top, low = a * top - b * low, d * low - c * top
                    out = [x[h] - first[h] * top - second[h] * low for h in range(2)]
                    out[half] = jnp.where(sub == r, top, jnp.where(sub == r + 1, low, out[half]))
                    return out

                for k in range(j + 2, 16):
                    own[k] = eliminate(own[k])
                panel = eliminate(panel)
            lines = [row_of(panel[j // 8], j % 8) for j in range(16)]
            for i in others:
                t = jnp.where(inside, 0.0, tiles[i])
                for j in range(16):
                    t = t - cols[i][j] * lines[j]
                tiles[i] = t
            tiles[mine[0]], tiles[mine[1]] = panel
        done, rest = jnp.concatenate(tiles, 0), halves[1 - p]
        here = (lanes >= 64 * p) & (lanes < 64 * p + 64)
        halves[p] = done
        halves[1 - p] = jnp.where(here, 0.0, rest) - nn(rest[:, 64 * p:64 * p + 64], done)
    return jnp.concatenate(halves, 0)


def thirds(x):
    first = x.astype(jnp.bfloat16).astype(jnp.float32)
    rest = x - first
    second = rest.astype(jnp.bfloat16).astype(jnp.float32)
    return first, second, rest - second


def left(x, axis=1):
    p, q, r = thirds(x)
    return jnp.concatenate([p, q, p, r, p, q], axis).astype(jnp.bfloat16)


def right(x, axis):
    p, q, r = thirds(x)
    return jnp.concatenate([q, q, r, p, p, p], axis).astype(jnp.bfloat16)


def nn(a, b):
    return jnp.dot(left(a), right(b, 0), preferred_element_type=jnp.float32)


def nt(a, b):
    return lax.dot_general(a, b, (((1,), (1,)), ((), ())), preferred_element_type=jnp.float32)


def factor_solve(h_ref, x_ref, n):
    blocks = n // NB

    def step(k, carry):
        at = pl.ds(pl.multiple_of(k * NB, NB), NB)
        inv = invert_block(h_ref[at, at])
        for kk in range(blocks):
            @pl.when(k == kk)
            def _(kk=kk):
                kc = slice(kk * NB, (kk + 1) * NB)
                s = (kk + 1) * NB
                below = h_ref[s:n + 8, kc]
                w = nn(below, inv)
                wide, tall = left(w), right(below, 1)
                c = s
                while c < n:
                    wd = min(256, n - c)
                    h_ref[c:n + 8, c:c + wd] -= nt(wide[c - s:, :], tall[c - s:c - s + wd, :])
                    c += wd
                h_ref[s:n + 8, kc] = w
        return carry

    lax.fori_loop(0, blocks, step, 0)
    for k in reversed(range(blocks)):
        kc = slice(k * NB, (k + 1) * NB)
        s = (k + 1) * NB
        y = h_ref[n:n + 8, kc]
        if s < n:
            y = y - nn(x_ref[:, s:], h_ref[s:n, kc])
        x_ref[:, kc] = y


def solve_kernel(total, parts, where_ref, *refs):
    halves, (g_ref, x_ref, s_ref, h_ref) = refs[: 2 * len(parts)], refs[2 * len(parts):]
    n = s_ref.shape[1]

    def place(j, carry):
        outer, inner = j >> 2, j & 3
        for i, (low, high, order) in enumerate(parts):
            at = [0, 0]
            at[order[0]] = (outer + where_ref[order[0]]) & 3
            at[order[1]] = (inner + where_ref[order[1]]) & 3
            for partner in range(2):
                src = halves[2 * i + partner]
                core = where_ref[3] ^ partner
                for last in range(4):
                    to = (((core * 4 + at[0]) * 4 + at[1]) * 4 + ((last + where_ref[2]) & 3)) * 16
                    to = pl.ds(pl.multiple_of(to, 16), 16)
                    for c in range(high - low):
                        start = pl.multiple_of((j * 4 + last) * ((high - low) * 16) + c * 16, 16)
                        s_ref[to, (low + c) * 128:(low + c + 1) * 128] = src[pl.ds(start, 16), :]
        return carry

    lax.fori_loop(0, 16, place, 0)
    for c in range(0, n, 256):
        gram = lax.dot_general(
            s_ref[:, c:], s_ref[:, c:c + 256], (((0,), (0,)), ((), ())), preferred_element_type=jnp.float32
        )
        r = lax.broadcasted_iota(jnp.int32, gram.shape, 0)
        q = lax.broadcasted_iota(jnp.int32, gram.shape, 1)
        h_ref[c:n, c:c + 256] = gram / total + jnp.where(r == q, ridge, 0.0)
    h_ref[n:n + 8, :] = jnp.broadcast_to(g_ref[...], (8, n))
    factor_solve(h_ref, x_ref, n)


def solve(pieces, gradient, where, total):
    n = gradient.shape[0]
    rows = 2 * 64 * 16
    vmem = pl.BlockSpec(memory_space=pltpu.VMEM)
    return pl.pallas_call(
        functools.partial(solve_kernel, total, PARTS),
        out_shape=jax.ShapeDtypeStruct((8, n), jnp.float32),
        in_specs=[pl.BlockSpec(memory_space=pltpu.SMEM)] + [vmem] * (len(pieces) + 1),
        out_specs=vmem,
        scratch_shapes=[pltpu.VMEM((rows, n), jnp.bfloat16), pltpu.VMEM((n + 8, n), jnp.float32)],
        compiler_params=pltpu.CompilerParams(vmem_limit_bytes=48 << 20),
        name="solve",
    )(where, *pieces, gradient[None, :])[0]


def reduce_over_devices(mine, other, grad):
    blocks, g = list(mine), grad
    count = grad.shape[0]

    def exchange(x, axis, k, with_grad):
        flat = x.reshape(-1, x.shape[-1])
        if not with_grad:
            return shift(flat, axis, k).reshape(x.shape), g
        got = shift(jnp.concatenate([flat, g], 0), axis, k)
        return got[:-count].reshape(x.shape), got[-count:]

    theirs = [exchange(other[i], 3, 1, False)[0] for i in range(len(PARTS))]
    g = g + shift(g, 3, 1)
    for i, (_, _, order) in enumerate(PARTS):
        axis = order[0]
        b = [sum(lax.index_in_dim(x, k, axis, False) for x in (mine[i], theirs[i])) for k in range(4)]
        up, up_g = exchange(b[2][:2], axis, 1, i == 1)
        down, down_g = exchange(b[2][2:], axis, 3, i == 1)
        near = jnp.concatenate([b[1][:2] + up, b[1][2:]], 0)
        far = jnp.concatenate([b[3][:2], b[3][2:] + down], 0)
        if i == 1:
            flat = shift(jnp.concatenate([near.reshape(-1, 128), up_g], 0), axis, 1)
            near, across_g = flat[:-count].reshape(near.shape), flat[-count:]
        else:
            near = shift(near.reshape(-1, 128), axis, 1).reshape(near.shape)
        far = shift(far.reshape(-1, 128), axis, 3).reshape(far.shape)
        blocks[i] = b[0] + (near + far)
    g = (g + across_g) + (up_g + down_g)
    for i, (_, _, order) in enumerate(PARTS):
        terms, terms_g = [blocks[i][0]], [g]
        for k in (1, 2, 3):
            got, got_g = exchange(blocks[i][k], order[1], k, i == 1)
            terms.append(got)
            terms_g.append(got_g)
        blocks[i] = sum_of_four(terms)
    g = sum_of_four(terms_g)
    both = jnp.concatenate(blocks, 1)
    terms, terms_g = [both], [g]
    for k in (1, 2, 3):
        got, got_g = exchange(both, 2, k, True)
        terms.append(jnp.roll(got, -k, 0))
        terms_g.append(got_g)
    both = sum_of_four(terms).astype(jnp.bfloat16)
    g = sum_of_four(terms_g)
    half = both.shape[1] // 2
    blocks = [both[:, :half].reshape(-1, 128), both[:, half:].reshape(-1, 128)]
    for stage in (1, 0):
        for i, (_, _, order) in enumerate(PARTS):
            got = [blocks[i]] + [shift(blocks[i], order[stage], k) for k in (3, 2, 1)]
            blocks[i] = jnp.concatenate(got, 0)
    pieces = []
    for b in blocks:
        pieces += [b, shift(b, 3, 1)]
    return pieces, g


def small_shift(x, stage, k):
    pairs = []
    for device in range(128):
        unit = (32, 8, 2)[2 - stage if device & 1 else stage]
        at = device // unit % 4
        pairs.append((device, device + ((at + k) % 4 - at) * unit))
    return lax.ppermute(x, ROWS, pairs)


def sum_over_devices(x):
    for stage in range(3):
        x = sum_of_four([x] + [small_shift(x, stage, k) for k in (1, 2, 3)])
    return x + shift(x, 3, 1)


def front_kernel(where_ref, at_ref, coef_ref, w_ref, code_ref, x_ref,
                 margin_ref, grad_ref, other_a_ref, other_b_ref, mine_a_ref, mine_b_ref, had_ref, mix_ref):
    step = pl.program_id(0)
    sub_blocks = x_ref.shape[0] // 256
    blocks = 16 // sub_blocks

    @pl.when(step == 0)
    def _():
        i = lax.broadcasted_iota(jnp.int32, (256, 256), 0)
        j = lax.broadcasted_iota(jnp.int32, (256, 256), 1)
        v = i & j
        v = v ^ (v >> 4)
        v = v ^ (v >> 2)
        v = (v ^ (v >> 1)) & 1
        had_ref[...] = jnp.where(v == 0, 1.0, -1.0).astype(jnp.bfloat16)
        grad_ref[...] = jnp.zeros_like(grad_ref)

    @pl.when(step < blocks)
    def _():
        low = jnp.broadcast_to(w_ref[...], (8, w_ref.shape[1])).astype(jnp.bfloat16)
        x = x_ref[...]
        margin = lax.dot_general(low, x, (((1,), (1,)), ((), ())), preferred_element_type=jnp.float32)
        prob = jax.nn.sigmoid(margin)
        code = code_ref[...]
        target = (code & 1).astype(jnp.float32)
        misfit = (prob - target).astype(jnp.bfloat16)
        spread = prob * (1.0 - prob)
        factor = jnp.where(spread > 0.0, jnp.sqrt(spread), 0.0)
        factor = (1 - (code & 2)).astype(jnp.float32) * factor
        margin_ref[...] = margin[:1, :]
        columns = [
            jnp.broadcast_to(factor[:1, sb * 256:(sb + 1) * 256], (128, 256)).T for sb in range(sub_blocks)
        ]
        for sb in range(sub_blocks):
            rows = slice(sb * 256, (sb + 1) * 256)
            for c in range(8):
                cols = slice(c * 128, (c + 1) * 128)
                scaled = (x_ref[rows, cols].astype(jnp.float32) * columns[sb]).astype(jnp.bfloat16)
                first = jnp.dot(had_ref[...], scaled, preferred_element_type=jnp.float32)
                at = (step * sub_blocks + sb) * 32
                mix_ref[pl.ds(at, 32), c * 8:(c + 1) * 8, :] = first.reshape(32, 8, 128)
        grad_ref[...] += jnp.dot(misfit, x_ref[...], preferred_element_type=jnp.float32)

    @pl.when(step == blocks)
    def _():
        def butterflies(t, carry):
            for c in range(8):
                cols = slice(c * 8, (c + 1) * 8)
                v = [mix_ref[t + 32 * k, cols, :] for k in range(16)]
                for bit in (1, 2, 4, 8):
                    v = [v[k] + v[k ^ bit] if not k & bit else v[k ^ bit] - v[k] for k in range(16)]
                for k in range(16):
                    mix_ref[t + 32 * k, cols, :] = v[k]
            return carry

        lax.fori_loop(0, 32, butterflies, 0)

    here = other_a_ref.shape[0]
    stages = 64 // here

    def pick_into(a_ref, b_ref, core, stage):
        flat = mix_ref.reshape(512 * 64, 128)

        def pick(i, carry):
            p = stage * here + i
            chip = 0
            for axis, bits in ((0, 4), (1, 2), (2, 0)):
                chip = chip * 4 + (((p >> bits) + where_ref[axis]) & 3)
            base = (chip * 2 + core) * 16
            for s in range(16):
                at = at_ref[base + s]
                coef = coef_ref[base + s]
                for out, start, count in ((a_ref, 0, 4), (b_ref, 32, 4)):
                    got = flat[pl.ds(at + start, count, stride=8), :]
                    out[i, pl.ds(s, count, stride=16), :] = got * coef
            return carry

        lax.fori_loop(0, here, pick, 0)

    @pl.when((step >= blocks) & (step < blocks + stages))
    def _():
        pick_into(other_a_ref, other_b_ref, 1 - where_ref[3], step - blocks)

    @pl.when(step >= blocks + stages)
    def _():
        pick_into(mine_a_ref, mine_b_ref, where_ref[3], step - blocks - stages)


def front(design, weights, labels, signs, rows, coefs, where):
    rows_here, width = design.shape
    block = 1024
    smem = pl.BlockSpec(memory_space=pltpu.SMEM)
    whole = lambda *shape: pl.BlockSpec(shape, lambda i: (0,) * len(shape))
    picked = [(64, 64, 128)] * 4
    blocks, stages = rows_here // block, 2
    at = (rows >> 3) * 64 + (rows & 7)
    shape = (64 // stages, 64, 128)
    first = pl.BlockSpec(shape, lambda i: (jnp.clip(i - blocks, 0, stages - 1), 0, 0))
    second = pl.BlockSpec(shape, lambda i: (jnp.clip(i - blocks - stages, 0, stages - 1), 0, 0))
    held = lambda i: jnp.minimum(i, blocks - 1)
    return pl.pallas_call(
        front_kernel,
        grid=(blocks + 2 * stages,),
        out_shape=[
            jax.ShapeDtypeStruct((1, rows_here), jnp.float32),
            jax.ShapeDtypeStruct((8, width), jnp.float32),
        ] + [jax.ShapeDtypeStruct(s, jnp.float32) for s in picked],
        in_specs=[
            smem, smem, smem,
            whole(1, width),
            pl.BlockSpec((1, block), lambda i: (0, held(i))),
            pl.BlockSpec((block, width), lambda i: (held(i), 0)),
        ],
        out_specs=[pl.BlockSpec((1, block), lambda i: (0, held(i))), whole(8, width)] + [first, first, second, second],
        scratch_shapes=[pltpu.VMEM((256, 256), jnp.bfloat16), pltpu.VMEM((512, 64, 128), jnp.float32)],
        compiler_params=pltpu.CompilerParams(vmem_limit_bytes=48 << 20),
        name="front",
    )(where, at, coefs, weights[None, :], (labels + 2 * signs)[None, :], design)


def body(design, weights, labels, signs, sample_rows):
    rows_here, width = design.shape
    device_count = lax.axis_size(ROWS)
    device_index = lax.axis_index(ROWS)
    where = jnp.stack([lax.axis_index(a) for a in ROWS])
    total_rows = rows_here * device_count
    norm_factor = 1.0 / jnp.sqrt(jnp.float32(sample_rows.shape[0]))
    parity = (sample_rows // rows_here) & device_index
    for bits in (4, 2, 1):
        parity = parity ^ (parity >> bits)
    coefs = (1 - 2 * (parity & 1)).astype(jnp.float32) * norm_factor
    margins, grad_part, *halves = front(
        design, weights, labels, signs, sample_rows % rows_here, coefs, where
    )
    halves = [h.reshape(4, 4, 4, -1, 128) for h in halves]
    pieces, grad = reduce_over_devices(halves[2:], halves[:2], grad_part[0].reshape(8, 128))
    gradient = grad.reshape(-1) / total_rows + ridge * weights
    newton_step = solve(pieces, gradient, where, float(total_rows))
    along = jnp.dot(design, newton_step.astype(jnp.bfloat16), preferred_element_type=jnp.float32)
    lengths = jnp.array([1.0, 0.5, 0.25, 0.125], jnp.float32)
    margins = margins[0]
    target = labels.astype(jnp.float32)
    trial = margins[None, :] - lengths[:, None] * along[None, :]
    row_loss = jnp.logaddexp(0.0, trial) - target[None, :] * trial
    loss_total = sum_over_devices(jnp.sum(row_loss, axis=1))
    moved = weights[None, :] - lengths[:, None] * newton_step[None, :]
    losses = loss_total / total_rows + 0.5 * ridge * jnp.sum(moved * moved, axis=1)
    return (gradient, newton_step, losses)


def solution(mesh):
    torus = Mesh(mesh.devices.reshape(4, 4, 4, 2), ROWS)
    in_specs = (P(ROWS, None), P(), P(ROWS), P(ROWS), P())
    out_specs = (P(), P(), P())
    return jax.shard_map(body, mesh=torus, in_specs=in_specs, out_specs=out_specs, check_vma=False)
```

```python
import functools

import jax
import jax.numpy as jnp
from jax import lax
from jax.experimental import pallas as pl
from jax.experimental.pallas import tpu as pltpu
from jax.sharding import Mesh
from jax.sharding import PartitionSpec as P

ROWS = ("rows_0", "rows_1", "rows_2", "rows_3")

ridge = 0.05

PARTS = ((0, 4, (0, 1)), (4, 8, (1, 0)))


def shift(x, axis, k):
    size = 2 if axis == 3 else 4
    return lax.ppermute(x, ROWS[axis], [(i, (i + k) % size) for i in range(size)])


def sum_of_four(x):
    return (x[0] + x[2]) + (x[1] + x[3])


NB = 128

def row_of(x, j):
    return jnp.broadcast_to(x[j:j + 1, :], x.shape)

def col_of(x, j):
    return jnp.broadcast_to(x[:, j:j + 1], x.shape)

def invert_block(block):
    lane = lax.broadcasted_iota(jnp.int32, (8, NB), 1)
    sub = lax.broadcasted_iota(jnp.int32, (8, NB), 0)
    lanes = lax.broadcasted_iota(jnp.int32, (64, NB), 1)
    real = lane < NB
    halves = [block[:64, :], block[64:, :]]
    for p in range(2):
        tiles = [halves[p][8 * t:8 * t + 8, :] for t in range(8)]
        for q in range(4):
            base = 64 * p + 16 * q
            inside = (lane >= base) & (lane < base + 16)
            mine = (2 * q, 2 * q + 1)
            others = [(2 * q + 2 + t) % 8 for t in range(6)]
            own = [[jnp.where(real, col_of(tiles[t], base + j), 0.0) for t in mine] for j in range(16)]
            cols = {i: [col_of(tiles[i], base + j) for j in range(16)] for i in others}
            panel = [
                jnp.where(inside, jnp.where(lane - base == sub + 8 * h, 1.0, 0.0), tiles[mine[h]]) for h in range(2)
            ]
            for j in range(0, 16, 2):
                half, r = j // 8, j % 8
                first, second = own[j], own[j + 1]
                a, b = row_of(first[half], r), row_of(second[half], r)
                c, d = row_of(first[half], r + 1), row_of(second[half], r + 1)
                inv = 1.0 / (a * d - b * c)
                a, b, c, d = d * inv, b * inv, c * inv, a * inv

                def eliminate(x):
                    top, low = row_of(x[half], r), row_of(x[half], r + 1)
                    top, low = a * top - b * low, d * low - c * top
                    out = [x[h] - first[h] * top - second[h] * low for h in range(2)]
                    out[half] = jnp.where(sub == r, top, jnp.where(sub == r + 1, low, out[half]))
                    return out

                for k in range(j + 2, 16):
                    own[k] = eliminate(own[k])
                panel = eliminate(panel)
            lines = [row_of(panel[j // 8], j % 8) for j in range(16)]
            for i in others:
                t = jnp.where(inside, 0.0, tiles[i])
                for j in range(16):
                    t = t - cols[i][j] * lines[j]
                tiles[i] = t
            tiles[mine[0]], tiles[mine[1]] = panel
        done, rest = jnp.concatenate(tiles, 0), halves[1 - p]
        here = (lanes >= 64 * p) & (lanes < 64 * p + 64)
        halves[p] = done
        halves[1 - p] = jnp.where(here, 0.0, rest) - nn(rest[:, 64 * p:64 * p + 64], done)
    return jnp.concatenate(halves, 0)


def thirds(x):
    first = x.astype(jnp.bfloat16).astype(jnp.float32)
    rest = x - first
    second = rest.astype(jnp.bfloat16).astype(jnp.float32)
    return first, second, rest - second


def left(x, axis=1):
    p, q, r = thirds(x)
    return jnp.concatenate([p, q, p, r, p, q], axis).astype(jnp.bfloat16)


def right(x, axis):
    p, q, r = thirds(x)
    return jnp.concatenate([q, q, r, p, p, p], axis).astype(jnp.bfloat16)


def nn(a, b):
    return jnp.dot(left(a), right(b, 0), preferred_element_type=jnp.float32)


def nt(a, b):
    return lax.dot_general(a, b, (((1,), (1,)), ((), ())), preferred_element_type=jnp.float32)


def factor_solve(h_ref, x_ref, n):
    blocks = n // NB

    def step(k, carry):
        at = pl.ds(pl.multiple_of(k * NB, NB), NB)
        inv = invert_block(h_ref[at, at])
        for kk in range(blocks):
            @pl.when(k == kk)
            def _(kk=kk):
                kc = slice(kk * NB, (kk + 1) * NB)
                s = (kk + 1) * NB
                below = h_ref[s:n + 8, kc]
                w = nn(below, inv)
                wide, tall = left(w), right(below, 1)
                c = s
                while c < n:
                    wd = min(256, n - c)
                    h_ref[c:n + 8, c:c + wd] -= nt(wide[c - s:, :], tall[c - s:c - s + wd, :])
                    c += wd
                h_ref[s:n + 8, kc] = w
        return carry

    lax.fori_loop(0, blocks, step, 0)
    for k in reversed(range(blocks)):
        kc = slice(k * NB, (k + 1) * NB)
        s = (k + 1) * NB
        y = h_ref[n:n + 8, kc]
        if s < n:
            y = y - nn(x_ref[:, s:], h_ref[s:n, kc])
        x_ref[:, kc] = y


def solve_kernel(total, parts, where_ref, *refs):
    halves, (g_ref, x_ref, s_ref, h_ref) = refs[: 2 * len(parts)], refs[2 * len(parts):]
    n = s_ref.shape[1]

    def place(j, carry):
        outer, inner = j >> 2, j & 3
        for i, (low, high, order) in enumerate(parts):
            at = [0, 0]
            at[order[0]] = (outer + where_ref[order[0]]) & 3
            at[order[1]] = (inner + where_ref[order[1]]) & 3
            for partner in range(2):
                src = halves[2 * i + partner]
                core = where_ref[3] ^ partner
                for last in range(4):
                    to = (((core * 4 + at[0]) * 4 + at[1]) * 4 + ((last + where_ref[2]) & 3)) * 16
                    to = pl.ds(pl.multiple_of(to, 16), 16)
                    for c in range(high - low):
                        start = pl.multiple_of((j * 4 + last) * ((high - low) * 16) + c * 16, 16)
                        s_ref[to, (low + c) * 128:(low + c + 1) * 128] = src[pl.ds(start, 16), :]
        return carry

    lax.fori_loop(0, 16, place, 0)
    for c in range(0, n, 256):
        gram = lax.dot_general(
            s_ref[:, c:], s_ref[:, c:c + 256], (((0,), (0,)), ((), ())), preferred_element_type=jnp.float32
        )
        r = lax.broadcasted_iota(jnp.int32, gram.shape, 0)
        q = lax.broadcasted_iota(jnp.int32, gram.shape, 1)
        h_ref[c:n, c:c + 256] = gram / total + jnp.where(r == q, ridge, 0.0)
    h_ref[n:n + 8, :] = jnp.broadcast_to(g_ref[...], (8, n))
    factor_solve(h_ref, x_ref, n)


def solve(pieces, gradient, where, total):
    n = gradient.shape[0]
    rows = 2 * 64 * 16
    vmem = pl.BlockSpec(memory_space=pltpu.VMEM)
    return pl.pallas_call(
        functools.partial(solve_kernel, total, PARTS),
        out_shape=jax.ShapeDtypeStruct((8, n), jnp.float32),
        in_specs=[pl.BlockSpec(memory_space=pltpu.SMEM)] + [vmem] * (len(pieces) + 1),
        out_specs=vmem,
        scratch_shapes=[pltpu.VMEM((rows, n), jnp.bfloat16), pltpu.VMEM((n + 8, n), jnp.float32)],
        compiler_params=pltpu.CompilerParams(vmem_limit_bytes=48 << 20),
        name="solve",
    )(where, *pieces, gradient[None, :])[0]


def reduce_over_devices(mine, other, grad):
    blocks, g = list(mine), grad
    count = grad.shape[0]

    def exchange(x, axis, k, with_grad):
        flat = x.reshape(-1, x.shape[-1])
        if not with_grad:
            return shift(flat, axis, k).reshape(x.shape), g
        got = shift(jnp.concatenate([flat, g], 0), axis, k)
        return got[:-count].reshape(x.shape), got[-count:]

    theirs = [exchange(other[i], 3, 1, False)[0] for i in range(len(PARTS))]
    for i, (_, _, order) in enumerate(PARTS):
        axis = order[0]
        b = [sum(lax.index_in_dim(x, k, axis, False) for x in (mine[i], theirs[i])) for k in range(4)]
        up, up_g = exchange(b[2][:2], axis, 1, i == 1)
        down, down_g = exchange(b[2][2:], axis, 3, i == 1)
        near = jnp.concatenate([b[1][:2] + up, b[1][2:]], 0)
        far = jnp.concatenate([b[3][:2], b[3][2:] + down], 0)
        if i == 1:
            flat = shift(jnp.concatenate([near.reshape(-1, 128), up_g], 0), axis, 1)
            near, across_g = flat[:-count].reshape(near.shape), flat[-count:]
        else:
            near = shift(near.reshape(-1, 128), axis, 1).reshape(near.shape)
        far = shift(far.reshape(-1, 128), axis, 3).reshape(far.shape)
        blocks[i] = b[0] + (near + far)
    g = (g + across_g) + (up_g + down_g)
    for i, (_, _, order) in enumerate(PARTS):
        terms, terms_g = [blocks[i][0]], [g]
        for k in (1, 2, 3):
            got, got_g = exchange(blocks[i][k], order[1], k, i == 1)
            terms.append(got)
            terms_g.append(got_g)
        blocks[i] = sum_of_four(terms)
    g = sum_of_four(terms_g)
    both = jnp.concatenate(blocks, 1)
    terms, terms_g = [both], [g]
    for k in (1, 2, 3):
        got, got_g = exchange(both, 2, k, True)
        terms.append(jnp.roll(got, -k, 0))
        terms_g.append(got_g)
    both = sum_of_four(terms).astype(jnp.bfloat16)
    g = sum_of_four(terms_g)
    g = g + shift(g, 3, 1)
    half = both.shape[1] // 2
    blocks = [both[:, :half].reshape(-1, 128), both[:, half:].reshape(-1, 128)]
    for stage in (1, 0):
        for i, (_, _, order) in enumerate(PARTS):
            got = [blocks[i]] + [shift(blocks[i], order[stage], k) for k in (3, 2, 1)]
            blocks[i] = jnp.concatenate(got, 0)
    pieces = []
    for b in blocks:
        pieces += [b, shift(b, 3, 1)]
    return pieces, g


def small_shift(x, stage, k):
    pairs = []
    for device in range(128):
        unit = (32, 8, 2)[2 - stage if device & 1 else stage]
        at = device // unit % 4
        pairs.append((device, device + ((at + k) % 4 - at) * unit))
    return lax.ppermute(x, ROWS, pairs)


def sum_over_devices(x):
    for stage in range(3):
        x = sum_of_four([x] + [small_shift(x, stage, k) for k in (1, 2, 3)])
    return x + shift(x, 3, 1)


def front_kernel(where_ref, at_ref, coef_ref, w_ref, code_ref, x_ref,
                 margin_ref, grad_ref, other_a_ref, other_b_ref, mine_a_ref, mine_b_ref, had_ref, mix_ref):
    step = pl.program_id(0)
    sub_blocks = x_ref.shape[0] // 256
    blocks = 16 // sub_blocks

    @pl.when(step == 0)
    def _():
        i = lax.broadcasted_iota(jnp.int32, (256, 256), 0)
        j = lax.broadcasted_iota(jnp.int32, (256, 256), 1)
        v = i & j
        v = v ^ (v >> 4)
        v = v ^ (v >> 2)
        v = (v ^ (v >> 1)) & 1
        had_ref[...] = jnp.where(v == 0, 1.0, -1.0).astype(jnp.bfloat16)
        grad_ref[...] = jnp.zeros_like(grad_ref)

    @pl.when(step < blocks)
    def _():
        low = jnp.broadcast_to(w_ref[...], (8, w_ref.shape[1])).astype(jnp.bfloat16)
        x = x_ref[...]
        margin = lax.dot_general(low, x, (((1,), (1,)), ((), ())), preferred_element_type=jnp.float32)
        prob = jax.nn.sigmoid(margin)
        code = code_ref[...]
        target = (code & 1).astype(jnp.float32)
        misfit = (prob - target).astype(jnp.bfloat16)
        spread = prob * (1.0 - prob)
        factor = jnp.where(spread > 0.0, jnp.sqrt(spread), 0.0)
        factor = (1 - (code & 2)).astype(jnp.float32) * factor
        margin_ref[...] = margin[:1, :]
        columns = [
            jnp.broadcast_to(factor[:1, sb * 256:(sb + 1) * 256], (128, 256)).T for sb in range(sub_blocks)
        ]
        for sb in range(sub_blocks):
            rows = slice(sb * 256, (sb + 1) * 256)
            for c in range(8):
                cols = slice(c * 128, (c + 1) * 128)
                scaled = (x_ref[rows, cols].astype(jnp.float32) * columns[sb]).astype(jnp.bfloat16)
                first = jnp.dot(had_ref[...], scaled, preferred_element_type=jnp.float32)
                at = (step * sub_blocks + sb) * 32
                mix_ref[pl.ds(at, 32), c * 8:(c + 1) * 8, :] = first.reshape(32, 8, 128)
        grad_ref[...] += jnp.dot(misfit, x_ref[...], preferred_element_type=jnp.float32)

    @pl.when(step == blocks)
    def _():
        def butterflies(t, carry):
            for c in range(8):
                cols = slice(c * 8, (c + 1) * 8)
                v = [mix_ref[t + 32 * k, cols, :] for k in range(16)]
                for bit in (1, 2, 4, 8):
                    v = [v[k] + v[k ^ bit] if not k & bit else v[k ^ bit] - v[k] for k in range(16)]
                for k in range(16):
                    mix_ref[t + 32 * k, cols, :] = v[k]
            return carry

        lax.fori_loop(0, 32, butterflies, 0)

    here = other_a_ref.shape[0]
    stages = 64 // here

    def pick_into(a_ref, b_ref, core, stage):
        flat = mix_ref.reshape(512 * 64, 128)

        def pick(i, carry):
            p = stage * here + i
            chip = 0
            for axis, bits in ((0, 4), (1, 2), (2, 0)):
                chip = chip * 4 + (((p >> bits) + where_ref[axis]) & 3)
            base = (chip * 2 + core) * 16
            for s in range(16):
                at = at_ref[base + s]
                coef = coef_ref[base + s]
                for out, start, count in ((a_ref, 0, 4), (b_ref, 32, 4)):
                    got = flat[pl.ds(at + start, count, stride=8), :]
                    out[i, pl.ds(s, count, stride=16), :] = got * coef
            return carry

        lax.fori_loop(0, here, pick, 0)

    @pl.when((step >= blocks) & (step < blocks + stages))
    def _():
        pick_into(other_a_ref, other_b_ref, 1 - where_ref[3], step - blocks)

    @pl.when(step >= blocks + stages)
    def _():
        pick_into(mine_a_ref, mine_b_ref, where_ref[3], step - blocks - stages)


def front(design, weights, labels, signs, rows, coefs, where):
    rows_here, width = design.shape
    block = 1024
    smem = pl.BlockSpec(memory_space=pltpu.SMEM)
    whole = lambda *shape: pl.BlockSpec(shape, lambda i: (0,) * len(shape))
    picked = [(64, 64, 128)] * 4
    blocks, stages = rows_here // block, 2
    at = (rows >> 3) * 64 + (rows & 7)
    shape = (64 // stages, 64, 128)
    first = pl.BlockSpec(shape, lambda i: (jnp.clip(i - blocks, 0, stages - 1), 0, 0))
    second = pl.BlockSpec(shape, lambda i: (jnp.clip(i - blocks - stages, 0, stages - 1), 0, 0))
    held = lambda i: jnp.minimum(i, blocks - 1)
    return pl.pallas_call(
        front_kernel,
        grid=(blocks + 2 * stages,),
        out_shape=[
            jax.ShapeDtypeStruct((1, rows_here), jnp.float32),
            jax.ShapeDtypeStruct((8, width), jnp.float32),
        ] + [jax.ShapeDtypeStruct(s, jnp.float32) for s in picked],
        in_specs=[
            smem, smem, smem,
            whole(1, width),
            pl.BlockSpec((1, block), lambda i: (0, held(i))),
            pl.BlockSpec((block, width), lambda i: (held(i), 0)),
        ],
        out_specs=[pl.BlockSpec((1, block), lambda i: (0, held(i))), whole(8, width)] + [first, first, second, second],
        scratch_shapes=[pltpu.VMEM((256, 256), jnp.bfloat16), pltpu.VMEM((512, 64, 128), jnp.float32)],
        compiler_params=pltpu.CompilerParams(vmem_limit_bytes=48 << 20),
        name="front",
    )(where, at, coefs, weights[None, :], (labels + 2 * signs)[None, :], design)


def body(design, weights, labels, signs, sample_rows):
    rows_here, width = design.shape
    device_count = lax.axis_size(ROWS)
    device_index = lax.axis_index(ROWS)
    where = jnp.stack([lax.axis_index(a) for a in ROWS])
    total_rows = rows_here * device_count
    norm_factor = 1.0 / jnp.sqrt(jnp.float32(sample_rows.shape[0]))
    parity = (sample_rows // rows_here) & device_index
    for bits in (4, 2, 1):
        parity = parity ^ (parity >> bits)
    coefs = (1 - 2 * (parity & 1)).astype(jnp.float32) * norm_factor
    margins, grad_part, *halves = front(
        design, weights, labels, signs, sample_rows % rows_here, coefs, where
    )
    halves = [h.reshape(4, 4, 4, -1, 128) for h in halves]
    pieces, grad = reduce_over_devices(halves[2:], halves[:2], grad_part[0].reshape(8, 128))
    gradient = grad.reshape(-1) / total_rows + ridge * weights
    newton_step = solve(pieces, gradient, where, float(total_rows))
    along = jnp.dot(design, newton_step.astype(jnp.bfloat16), preferred_element_type=jnp.float32)
    lengths = jnp.array([1.0, 0.5, 0.25, 0.125], jnp.float32)
    margins = margins[0]
    target = labels.astype(jnp.float32)
    trial = margins[None, :] - lengths[:, None] * along[None, :]
    row_loss = jnp.logaddexp(0.0, trial) - target[None, :] * trial
    loss_total = sum_over_devices(jnp.sum(row_loss, axis=1))
    moved = weights[None, :] - lengths[:, None] * newton_step[None, :]
    losses = loss_total / total_rows + 0.5 * ridge * jnp.sum(moved * moved, axis=1)
    return (gradient, newton_step, losses)


def solution(mesh):
    torus = Mesh(mesh.devices.reshape(4, 4, 4, 2), ROWS)
    in_specs = (P(ROWS, None), P(), P(ROWS), P(ROWS), P())
    out_specs = (P(), P(), P())
    return jax.shard_map(body, mesh=torus, in_specs=in_specs, out_specs=out_specs, check_vma=False)
```
